32 devices in a mesh: gx: 16 (over z, y, core), gy: 2 (over x).
Axes of the slice: x: 2, y: 2, z: 4, core: 2. Of those that a mesh axis runs over, the one named last changes fastest.
Arguments:
- right_side: float32 [16, 2, 512, 256], P('gx', 'gy'), may hold values from -8 to 8, as said below
- coords: float32 [16, 2, 2, 512], P('gx', 'gy'), may hold values from 0 to 1
- noise: float32 [16, 2, 512], P('gx', 'gy'), may hold values from 0.25 to 1
- intersect: int32 [16, 2, 128], P('gx', 'gy'), may hold values from 0 to 4607, as said below
Outputs:
- solution: float32 [16, 2, 512, 256], P('gx', 'gy')
- residual: float32 [16, 2, 512, 256], P('gx', 'gy')
The draws below stay inside these ranges and needn't reach their ends.
Inputs may be any that keep to these rules, and one draw needn't show every extreme that they name: `right_side`: right-hand sides of order one. `intersect`: each subdomain's list holds 128 distinct indices in increasing order; none names the subdomain itself (block number 4) or a subdomain beyond the first or last one along the second dimension.
All inputs are finite; a program needn't handle non-finite values.
Results may differ from the reference program's by a relative error of at most 0.0003.
Values sent between devices are 32-bit elements; how exact they have to be, the bound alone decides.
A program may use at most 128 MiB of HBM per device.

```python
import math
import jax
import jax.numpy as jnp
from jax import lax

P_SIZE = 512
OV = 128
R = 256
ITERS = 3
CELLS_X = 16
CELLS_Y = 2


def draw_right_side(key, part):
    full_shape = (CELLS_X, CELLS_Y, P_SIZE, R)
    normal_vals = jax.random.normal(key, full_shape, jnp.float32)
    return jnp.clip(normal_vals, -6.0, 6.0)


def draw_intersect(key, part):
    slot_count = 9 * P_SIZE

    def per_cell(cell_id):
        cell_key = jax.random.fold_in(key, cell_id + 7)
        column_id = cell_id % CELLS_Y
        slot_ids = jnp.arange(slot_count, dtype=jnp.int32)
        block_col = slot_ids // P_SIZE % 3
        banned = (slot_ids // P_SIZE == 4) | (block_col == 0) & (column_id == 0) | (block_col == 2) & (column_id == CELLS_Y - 1)
        scores = jax.random.randint(cell_key, (slot_count,), 0, 131072, dtype=jnp.int32) * slot_count + slot_ids
        scores = jnp.where(banned, 1073741824 + slot_ids, scores)
        ranking = jnp.argsort(scores, stable=True)
        return jnp.sort(ranking[:OV]).astype(jnp.int32)
    chosen = jax.vmap(per_cell)(jnp.arange(CELLS_X * CELLS_Y, dtype=jnp.int32))
    return chosen.reshape(CELLS_X, CELLS_Y, OV)


def steps_of(stream_key, shape, shards, smallest, high):
    def one(position, parts):
        heights = jax.random.uniform(jax.random.fold_in(jax.random.fold_in(stream_key, 6), position), (parts,), jnp.float32, smallest / len(shards), high / len(shards))
        return jnp.repeat(jnp.exp(heights), shape[position] // parts).reshape((-1,) + (1,) * (len(shape) - position - 1))

    level = one(*shards[0])
    for cut in shards[1:]:
        level = level * one(*cut)
    return level


def setup_inputs(seed: int = 0) -> dict:
    keys = jax.random.split(jax.random.key(seed), 5)
    right_side = draw_right_side(jax.random.fold_in(keys[4], 71), 0)
    coords = jnp.clip(1.0 * jax.random.uniform(keys[1], (CELLS_X, CELLS_Y, 2, P_SIZE), jnp.float32) ** steps_of(keys[1], (CELLS_X, CELLS_Y, 2, P_SIZE), ((0, 16), (1, 2)), -0.2, 0.2), 0.0, 1.0)
    noise = jnp.clip(jnp.exp(math.log(1.0) - 1.3862944 * jax.random.uniform(keys[2], (CELLS_X, CELLS_Y, P_SIZE), jnp.float32) ** steps_of(keys[2], (CELLS_X, CELLS_Y, P_SIZE), ((0, 16), (1, 2)), -0.2, 0.2)), 0.25, 1.0)
    intersect = draw_intersect(jax.random.fold_in(keys[4], 71), 0)
    return {"right_side": right_side, "coords": coords, "noise": noise, "intersect": intersect}


RANGE_LEN = 0.25
ROOT_THREE = math.sqrt(3.0)
HIGH = lax.Precision.HIGHEST

def kernel_block(rows_pos, cols_pos):
    delta_x = rows_pos[0][:, None] - cols_pos[0][None, :]
    delta_y = rows_pos[1][:, None] - cols_pos[1][None, :]
    distance = jnp.sqrt(delta_x * delta_x + delta_y * delta_y)
    scaled = ROOT_THREE / RANGE_LEN * distance
    clipped = jnp.minimum(distance, 1.0)
    taper_val = jnp.square(jnp.square(1.0 - clipped)) * (4.0 * clipped + 1.0)
    return (1.0 + scaled) * jnp.exp(-scaled) * taper_val

def reference(right_side, coords, noise, intersect):
    cells_x, cells_y, points, rhs_count = right_side.shape
    intersect_len = intersect.shape[2]
    cell_count = cells_x * cells_y
    ext_len = points + intersect_len

    def neighbour(values, cell_row, cell_col, shift_x, shift_y):
        near_row = (cell_row + shift_x) % cells_x
        near_col = cell_col + shift_y
        inside = (near_col >= 0) & (near_col < cells_y)
        fetched = values[near_row, jnp.clip(near_col, 0, cells_y - 1)]
        return jnp.where(inside, fetched, jnp.zeros_like(fetched))

    def operate(vector):

        def per_cell(cell_id):
            cell_row = cell_id // cells_y
            cell_col = cell_id % cells_y
            own_pos = coords[cell_row, cell_col]
            accumulated = noise[cell_row, cell_col][:, None] * vector[cell_row, cell_col]
            for shift_x in (-1, 0, 1):
                for shift_y in (-1, 0, 1):
                    near_info = neighbour(coords, cell_row, cell_col, shift_x, shift_y)
                    near_pos = jnp.stack([near_info[0] + float(shift_x), near_info[1] + float(shift_y)])
                    near_vec = neighbour(vector, cell_row, cell_col, shift_x, shift_y)
                    accumulated = accumulated + jnp.dot(kernel_block(own_pos, near_pos).astype(jnp.float32), near_vec.astype(jnp.float32), precision=HIGH, preferred_element_type=jnp.float32)
            return accumulated
        result = lax.map(per_cell, jnp.arange(cell_count, dtype=jnp.int32))
        return result.reshape(cells_x, cells_y, points, rhs_count)

    def setup_cell(cell_id):
        cell_row = cell_id // cells_y
        cell_col = cell_id % cells_y
        intersect_ids = intersect[cell_row, cell_col]
        block_id = intersect_ids // points
        row_in = intersect_ids % points
        row_of = block_id // 3
        col_of = block_id % 3
        near_row = ((cell_row + row_of - 1) % cells_x).astype(jnp.int32)
        near_col = (cell_col + col_of - 1).astype(jnp.int32)
        pos_x = coords[near_row, near_col, 0, row_in]
        pos_y = coords[near_row, near_col, 1, row_in]
        ov_pos = jnp.stack([pos_x + (row_of - 1).astype(jnp.float32), pos_y + (col_of - 1).astype(jnp.float32)])
        ext_pos = jnp.concatenate([coords[cell_row, cell_col], ov_pos], axis=1)
        ext_noise = jnp.concatenate([noise[cell_row, cell_col], noise[near_row, near_col, row_in]])
        local_matrix = kernel_block(ext_pos, ext_pos) + jnp.diag(ext_noise)
        factor = jnp.linalg.cholesky(local_matrix)
        inv_factor = lax.linalg.triangular_solve(factor, jnp.eye(ext_len, dtype=jnp.float32), left_side=True, lower=True)
        inverse = jnp.dot(inv_factor.T.astype(jnp.float32), inv_factor.astype(jnp.float32), precision=HIGH, preferred_element_type=jnp.float32)
        global_ids = ((near_row * cells_y + near_col) * points + row_in).astype(jnp.int32)
        return (inverse, global_ids)
    inverses, global_ids = lax.map(setup_cell, jnp.arange(cell_count, dtype=jnp.int32))

    def precondition(residue):
        flat_res = residue.reshape(cell_count * points, rhs_count)
        extended = jnp.concatenate([residue.reshape(cell_count, points, rhs_count), flat_res[global_ids]], axis=1)
        solved = jnp.einsum('cij,cjr->cir', inverses, extended, precision=HIGH)
        result = solved[:, :points].reshape(cell_count * points, rhs_count)
        result = result.at[global_ids.reshape(-1)].add(solved[:, points:].reshape(-1, rhs_count))
        return result.reshape(cells_x, cells_y, points, rhs_count)

    def column_sum(first, second):
        return lax.optimization_barrier(jnp.sum(first * second, axis=(0, 1, 2)))
    solution = jnp.zeros_like(right_side)
    residual = right_side
    precond = precondition(residual)
    direction = precond
    inner_now = column_sum(residual, precond)
    for iteration in range(ITERS):
        image_vec = operate(direction)
        step_size = inner_now / column_sum(direction, image_vec)
        solution = solution + step_size * direction
        residual = residual - step_size * image_vec
        if iteration + 1 < ITERS:
            precond = precondition(residual)
            inner_next = column_sum(residual, precond)
            direction = precond + inner_next / inner_now * direction
            inner_now = inner_next
    return (solution, residual)
```

```python
import functools
import math

import jax
import jax.numpy as jnp
from jax import lax
from jax.experimental import pallas as pl
from jax.experimental.pallas import tpu as pltpu
from jax.sharding import PartitionSpec as P

ITERS = 3


RANGE_LEN = 0.25
ROOT_THREE = math.sqrt(3.0)
HIGH = lax.Precision.HIGHEST


def shifted(value, axis, by):
    count = lax.axis_size(axis)
    return lax.ppermute(value, axis, [(i, (i + by) % count) for i in range(count)])


def passed_along(block, axis, distance):
    devices = range(lax.axis_size(axis))
    route = [(i - distance, i) for i in devices if i - distance in devices]
    return lax.ppermute(block, axis, route)


def kernel_block(rows_pos, cols_pos):
    delta_x = rows_pos[0][:, None] - cols_pos[0][None, :]
    delta_y = rows_pos[1][:, None] - cols_pos[1][None, :]
    distance = jnp.sqrt(delta_x * delta_x + delta_y * delta_y)
    scaled = ROOT_THREE / RANGE_LEN * distance
    clipped = jnp.minimum(distance, 1.0)
    taper_val = jnp.square(jnp.square(1.0 - clipped)) * (4.0 * clipped + 1.0)
    return (1.0 + scaled) * jnp.exp(-scaled) * taper_val


def window_values(values):
    beside = {}
    for step_by in (1, -1):
        beside[step_by] = shifted(values, "gx", step_by)
    column = jnp.stack([beside[1], values, beside[-1]])
    across = {}
    for step_by in (1, -1):
        across[step_by] = passed_along(column, "gy", step_by)
    return [across[1], column, across[-1]]


CHUNKS = 4
MESH = pl.DeviceIdType.MESH
NOISE_MIN = 0.25
VMEM = pl.BlockSpec(memory_space=pltpu.VMEM)


def split(value):
    top = value.astype(jnp.bfloat16)
    return top, (value - top.astype(jnp.float32)).astype(jnp.bfloat16)


def dot3(left, right):
    left_top, left_low = split(left)
    right_top, right_low = split(right)
    return jnp.dot(
        jnp.concatenate([left_top, left_top, left_low], axis=1),
        jnp.concatenate([right_top, right_low, right_top], axis=0),
        preferred_element_type=jnp.float32,
    )


def dot6(left, right):
    return jnp.dot(left, right, precision=HIGH, preferred_element_type=jnp.float32)


def block_inverse(block):
    size = block.shape[0]
    low, high = NOISE_MIN * 0.97, (size + 1.0) * 1.01
    eye = (
        lax.broadcasted_iota(jnp.int32, block.shape, 0)
        == lax.broadcasted_iota(jnp.int32, block.shape, 1)
    ).astype(jnp.float32)
    first = 2.0 / (low + high)
    gap = 1.0 - first * low
    scale = 2.0 / (2.0 - gap * gap)
    guess = (2.0 * first * scale) * eye - (first * first * scale) * block
    gap = gap * gap / (2.0 - gap * gap)
    while gap > 1e-3:
        scale = 2.0 / (2.0 - gap * gap)
        rest = 2.0 * eye - dot3(block, guess)
        guess = scale * dot3(guess, rest)
        gap = gap * gap / (2.0 - gap * gap)
    for _ in range(2):
        guess = guess + dot3(guess, eye - dot6(block, guess))
    return guess


def invert(matrix_ref, out_ref):
    size = matrix_ref.shape[0]
    step = math.gcd(size, 128)
    out_ref[...] = matrix_ref[...]
    for start in range(0, size, step):
        here = slice(start, start + step)
        pivot = block_inverse(out_ref[here, here])
        column = out_ref[:, here]
        row = dot6(pivot, out_ref[here, :])
        for low in range(0, size, step):
            if low != start:
                part = slice(low, low + step)
                out_ref[part, :] = out_ref[part, :] - dot6(column[part], row)
                out_ref[part, here] = -dot6(column[part], pivot)
        out_ref[here, :] = row
        out_ref[here, here] = pivot


def columns_of(count):
    return () if count == 1 else (1,) if count == 2 else (-1, 1)


def opposite(col_off, count):
    return col_off if count == 2 else -col_off


def offsets_of(count):
    near = [(-1, 0), (1, 0)]
    for col_off in columns_of(count):
        near += [(0, col_off), (-1, col_off), (1, col_off)]
    return near


def cg_kernel(
    rhs_ref, window_ref, matrix_ref, pick_ref, put_ref,
    solution_ref, residual_ref,
    top_ref, low_ref, inverse, inv_top_ref, inv_low_ref, asked, got, tail, back, precond, window, direction, image, mine, slots_y, slots_x,
    send_sem, recv_sem,
):
    size_x, size_y = lax.axis_size("gx"), lax.axis_size("gy")
    my_x, my_y = lax.axis_index("gx"), lax.axis_index("gy")
    near = offsets_of(size_y)
    points = rhs_ref.shape[0]
    borrowed = tail.shape[0]
    half = points // CHUNKS

    def inside(col_off):
        if col_off == 0 or size_y == 2:
            return None
        return my_y > 0 if col_off < 0 else my_y < size_y - 1

    def guarded(condition, action):
        if condition is None:
            action()
        else:
            pl.when(condition)(action)

    def target(row_off, col_off):
        place = {}
        if row_off:
            place["gx"] = lax.rem(my_x + row_off + size_x, size_x)
        if col_off:
            place["gy"] = 1 - my_y if size_y == 2 else my_y + col_off
        return place

    counter = [0]

    class Move:
        def __init__(self, source, dest, row_off, col_off):
            index = counter[0]
            counter[0] += 1
            self.copy = pltpu.make_async_remote_copy(
                src_ref=source,
                dst_ref=dest,
                send_sem=send_sem.at[index],
                recv_sem=recv_sem.at[index],
                device_id=target(row_off, col_off),
                device_id_type=MESH,
            )
            self.out = inside(col_off)
            self.into = inside(-col_off)

        def start(self):
            guarded(self.out, self.copy.start)

        def sent(self):
            guarded(self.out, self.copy.wait_send)

        def landed(self):
            guarded(self.into, self.copy.wait_recv)

    def slot(row_off, col_off):
        return near.index((-row_off, opposite(col_off, size_y)))

    barrier = pltpu.get_barrier_semaphore()
    greeted = 0
    for axis, here, count in (("gx", my_x, size_x), ("gy", my_y, size_y)):
        for hop in range(1, count):
            pl.semaphore_signal(
                barrier, inc=1, device_id={axis: lax.rem(here + hop, count)}, device_id_type=MESH
            )
            greeted += 1
    for row_off, col_off in near:
        if row_off and col_off:

            def greet(row_off=row_off, col_off=col_off):
                pl.semaphore_signal(
                    barrier, inc=1, device_id=target(row_off, col_off), device_id_type=MESH
                )

            guarded(inside(col_off), greet)
            there = inside(col_off)
            greeted = greeted + (1 if there is None else jnp.where(there, 1, 0))

    for col_off in columns_of(size_y):
        there = inside(col_off)
        if there is not None:

            def clear(col_off=col_off):
                for index, (_, col) in enumerate(near):
                    if col == col_off:
                        for iteration in range(ITERS):
                            got[iteration, index] = jnp.zeros(tail.shape, jnp.float32)
                            back[iteration, index] = jnp.zeros(tail.shape, jnp.float32)
                            window[iteration, index] = jnp.zeros(rhs_ref.shape, jnp.float32)

            pl.when(jnp.logical_not(there))(clear)

    def exact_dot(ones, value):
        top, low = split(value)
        return jnp.dot(ones, top, preferred_element_type=jnp.float32) + jnp.dot(
            ones, low, preferred_element_type=jnp.float32
        )

    def dot_parts(left_top, left_low, right):
        right_top, right_low = split(right)
        return (
            jnp.dot(left_top, right_top, preferred_element_type=jnp.float32)
            + jnp.dot(left_top, right_low, preferred_element_type=jnp.float32)
            + jnp.dot(left_low, right_top, preferred_element_type=jnp.float32)
        )

    def window_part(block, value):
        cols = slice(block * points, (block + 1) * points)
        return dot_parts(top_ref[:, cols], low_ref[:, cols], value)

    def total(iteration):
        for stage, (axis, here, count, slots) in enumerate(
            (("gy", my_y, size_y, slots_y), ("gx", my_x, size_x, slots_x))
        ):
            index = counter[0]
            counter[0] += 1
            for hop in range(1, count):
                pltpu.make_async_remote_copy(
                    src_ref=mine.at[iteration, stage],
                    dst_ref=slots.at[iteration, hop - 1],
                    send_sem=send_sem.at[index],
                    recv_sem=recv_sem.at[index],
                    device_id={axis: lax.rem(here + hop, count)},
                    device_id_type=MESH,
                ).start()
            so_far = mine[iteration, stage]
            if count > 1:
                held = slots.at[iteration]
                pltpu.make_async_copy(held, held, recv_sem.at[index]).wait()
                so_far = so_far + jnp.sum(slots[iteration], axis=0)
                pltpu.make_async_copy(held, held, send_sem.at[index]).wait()
            mine[iteration, stage + 1] = so_far
        return mine[iteration, 2]

    residual_ref[...] = rhs_ref[...]
    wait_entry = [True]
    inner_old = denominator = None
    for iteration in range(ITERS):
        requests = exact_dot(pick_ref[...], residual_ref[...])
        for index in range(len(near)):
            asked[index] = requests[index * borrowed : (index + 1) * borrowed]
        if wait_entry[0]:
            pl.semaphore_wait(barrier, greeted)
            wait_entry[0] = False
        moves = [
            Move(asked.at[index], got.at[iteration, slot(*offset)], *offset)
            for index, offset in enumerate(near)
        ]
        for move in moves:
            move.start()
        if iteration == 0:
            invert(matrix_ref, inverse)
            inv_top_ref[...], inv_low_ref[...] = split(inverse[...])
            top_ref[...], low_ref[...] = split(window_ref[...])
        solved = dot_parts(
            inv_top_ref[:, :points], inv_low_ref[:, :points], residual_ref[...]
        )
        for move in moves:
            move.landed()
        gathered = jnp.sum(got[iteration], axis=0)
        solved = solved + dot_parts(inv_top_ref[:, points:], inv_low_ref[:, points:], gathered)
        tail[...] = solved[points:]
        precond[...] = solved[:points]
        returns = [Move(tail, back.at[iteration, slot(*offset)], *offset) for offset in near]
        for move in returns:
            move.start()
        for move in moves:
            move.sent()
        for move in returns:
            move.landed()
        returned = back[iteration].reshape(len(near) * borrowed, tail.shape[1])
        precond[...] = precond[...] + exact_dot(put_ref[...], returned)
        for move in returns:
            move.sent()

        sides, relays = [], []
        for chunk in range(CHUNKS):
            rows = pl.ds(chunk * half, half)
            for col_off in columns_of(size_y):
                index = slot(0, col_off)
                sides.append(
                    Move(precond.at[rows], window.at[iteration, index, rows], 0, col_off)
                )
                sides[-1].start()
        beside = [
            Move(precond, window.at[iteration, slot(row_off, 0)], row_off, 0)
            for row_off in (-1, 1)
        ]
        for move in beside:
            move.start()
        result = window_part(len(near), precond[...])
        place = 0
        for chunk in range(CHUNKS):
            rows = pl.ds(chunk * half, half)
            for col_off in columns_of(size_y):
                sides[place].landed()
                place += 1
                source = near.index((0, opposite(col_off, size_y)))
                for row_off in (-1, 1):
                    index = near.index((-row_off, opposite(col_off, size_y)))
                    move = Move(
                        window.at[iteration, source, rows],
                        window.at[iteration, index, rows],
                        row_off,
                        0,
                    )
                    there = inside(-col_off)
                    move.out = move.into = there
                    relays.append(move)
                    move.start()
        for index, (row_off, col_off) in enumerate(near):
            if row_off == 0:
                result = result + window_part(index, window[iteration, index])
        for move in beside:
            move.landed()
        for index, (row_off, col_off) in enumerate(near):
            if row_off and col_off == 0:
                result = result + window_part(index, window[iteration, index])
        for move in relays:
            move.landed()
        for index, (row_off, col_off) in enumerate(near):
            if row_off and col_off:
                result = result + window_part(index, window[iteration, index])
        fresh = precond[...]
        mine[iteration, 0, 0:1] = jnp.sum(residual_ref[...] * fresh, axis=0, keepdims=True)
        mine[iteration, 0, 1:2] = jnp.sum(fresh * result, axis=0, keepdims=True)
        if iteration:
            mine[iteration, 0, 2:3] = jnp.sum(fresh * image[...], axis=0, keepdims=True)
        else:
            mine[iteration, 0, 2:3] = jnp.zeros((1, fresh.shape[1]), jnp.float32)
        sums = total(iteration)
        for move in sides + beside + relays:
            move.sent()
        inner, curved, mixed = sums[0:1], sums[1:2], sums[2:3]
        if iteration:
            ratio = inner / inner_old
            denominator = curved + ratio * (2.0 * mixed + ratio * denominator)
            direction[...] = fresh + ratio * direction[...]
            image[...] = result + ratio * image[...]
        else:
            denominator = curved
            direction[...] = fresh
            image[...] = result
        inner_old = inner
        step_size = inner / denominator
        moved = step_size * direction[...]
        solution_ref[...] = solution_ref[...] + moved if iteration else moved
        residual_ref[...] = residual_ref[...] - step_size * image[...]


def conjugate_gradients(right_side, window_matrix, matrix, pick):
    near = offsets_of(lax.axis_size("gy"))
    points, width = right_side.shape
    borrowed = matrix.shape[0] - points
    size_x, size_y = lax.axis_size("gx"), lax.axis_size("gy")
    sides = len(columns_of(size_y))
    moves = ITERS * (2 * len(near) + 2 + 3 * CHUNKS * sides + 2)
    out = jax.ShapeDtypeStruct(right_side.shape, jnp.float32)
    block = pltpu.VMEM((points, width), jnp.float32)
    small = (len(near), borrowed, width)
    return pl.pallas_call(
        cg_kernel,
        out_shape=(out, out),
        in_specs=[VMEM] * 5,
        out_specs=(VMEM, VMEM),
        scratch_shapes=[
            pltpu.VMEM(window_matrix.shape, jnp.bfloat16),
            pltpu.VMEM(window_matrix.shape, jnp.bfloat16),
            pltpu.VMEM(matrix.shape, jnp.float32),
            pltpu.VMEM(matrix.shape, jnp.bfloat16),
            pltpu.VMEM(matrix.shape, jnp.bfloat16),
            pltpu.VMEM(small, jnp.float32),
            pltpu.VMEM((ITERS,) + small, jnp.float32),
            pltpu.VMEM((borrowed, width), jnp.float32),
            pltpu.VMEM((ITERS,) + small, jnp.float32),
            block,
            pltpu.VMEM((ITERS, len(near), points, width), jnp.float32),
            block,
            block,
            pltpu.VMEM((ITERS, 3, 3, width), jnp.float32),
            pltpu.VMEM((ITERS, max(size_y - 1, 1), 3, width), jnp.float32),
            pltpu.VMEM((ITERS, max(size_x - 1, 1), 3, width), jnp.float32),
            pltpu.SemaphoreType.DMA((moves,)),
            pltpu.SemaphoreType.DMA((moves,)),
        ],
        compiler_params=pltpu.CompilerParams(
            collective_id=0, has_side_effects=True, vmem_limit_bytes=56 * 1024 * 1024
        ),
    )(right_side, window_matrix, matrix, pick, pick.T)


def shards(right_side, coords, noise, intersect):
    points = right_side.shape[2]
    rhs_count = right_side.shape[3]
    intersect_len = intersect.shape[2]
    ext_len = points + intersect_len
    own_pos = coords.reshape(2, points)
    own_noise = noise.reshape(points)
    listed = jnp.pad(intersect.reshape(intersect_len), (0, points - intersect_len))
    point_info = jnp.concatenate(
        [own_pos, own_noise[None, :], listed.astype(jnp.float32)[None, :]], axis=0
    )
    info_cols = window_values(point_info)
    intersect_ids = intersect.reshape(intersect_len)
    block_id = intersect_ids // points
    row_in = intersect_ids % points
    row_of = block_id // 3
    col_of = block_id % 3
    local_id = row_of * points + row_in
    picked_info = [
        jnp.take(
            jnp.transpose(info_cols[col_off], (1, 0, 2)).reshape(4, 3 * points), local_id, axis=1
        )
        for col_off in range(3)
    ]
    chosen = jnp.where(
        col_of[None, :] == 0,
        picked_info[0],
        jnp.where(col_of[None, :] == 1, picked_info[1], picked_info[2]),
    )
    ov_pos = jnp.stack(
        [chosen[0] + (row_of - 1).astype(jnp.float32), chosen[1] + (col_of - 1).astype(jnp.float32)]
    )
    ext_pos = jnp.concatenate([own_pos, ov_pos], axis=1)
    ext_noise = jnp.concatenate([own_noise, chosen[2]])
    local_matrix = kernel_block(ext_pos, ext_pos) + jnp.diag(ext_noise)
    count = lax.axis_size("gy")
    point_iota = jnp.arange(points, dtype=jnp.int32)[None, :]
    blocks, picks = [], []
    for row_off, col_off in offsets_of(count) + [(0, 0)]:
        step = col_off
        info = info_cols[col_off + 1][row_off + 1]
        if col_off and count == 2:
            first = lax.axis_index("gy") == 0
            step = jnp.where(first, 1, -1)
            info = jnp.where(first, info, info_cols[0][row_off + 1])
        shift = jnp.asarray(step, jnp.float32)
        blocks.append(
            kernel_block(own_pos, jnp.stack([info[0] + float(row_off), info[1] + shift]))
        )
        if row_off or col_off:
            ids = info[3, :intersect_len].astype(jnp.int32)
            own_rows = ids - (3 * (1 - row_off) + (1 - step)) * points
            picks.append((own_rows[:, None] == point_iota).astype(jnp.bfloat16))
    blocks[-1] = blocks[-1] + jnp.diag(own_noise)
    answer, residual = conjugate_gradients(
        right_side.reshape(points, rhs_count),
        jnp.concatenate(blocks, axis=1),
        local_matrix,
        jnp.concatenate(picks, axis=0),
    )
    return (answer.reshape(1, 1, points, rhs_count), residual.reshape(1, 1, points, rhs_count))


def split3(value):
    top = value.astype(jnp.bfloat16)
    rest = value - top.astype(jnp.float32)
    mid = rest.astype(jnp.bfloat16)
    return top, mid, (rest - mid.astype(jnp.float32)).astype(jnp.bfloat16)


def full_dot(left, right):
    lt, lm, ll = split3(left)
    rt, rm, rl = split3(right)
    return jnp.dot(
        jnp.concatenate([lt, lt, lm, lm, lt, ll], axis=1),
        jnp.concatenate([rt, rm, rt, rm, rl, rt], axis=0),
        preferred_element_type=jnp.float32,
    )


def wide(value):
    return jnp.concatenate(split(value), axis=1)


def folded(value):
    lanes = value.shape[1] // 2
    return value[:, :lanes] + value[:, lanes:]


def mm(left, right):
    return jnp.dot(left, right, preferred_element_type=jnp.float32)


def covariance(rows_x, rows_y, cols_x, cols_y):
    delta_x = rows_x - cols_x
    delta_y = rows_y - cols_y
    square = delta_x * delta_x + delta_y * delta_y
    distance = square * lax.rsqrt(jnp.maximum(square, 1e-30))
    scaled = ROOT_THREE / RANGE_LEN * distance
    rest = 1.0 - jnp.minimum(distance, 1.0)
    rest = rest * rest
    taper = rest * rest * (4.0 * jnp.minimum(distance, 1.0) + 1.0)
    return (1.0 + scaled) * jnp.exp(-scaled) * taper


def pivot_inverses(blocks):
    size = blocks[0].shape[0]
    low, high = NOISE_MIN * 0.97, (size + 1.0) * 1.01
    eye = (
        lax.broadcasted_iota(jnp.int32, blocks[0].shape, 0)
        == lax.broadcasted_iota(jnp.int32, blocks[0].shape, 1)
    ).astype(jnp.float32)
    first = 2.0 / (low + high)
    gap = 1.0 - first * low
    rests = [eye - first * block for block in blocks]
    scale = 2.0 / (2.0 - gap * gap)
    guesses = [(scale * first) * (eye + rest) for rest in rests]
    rests = [scale * full_dot(rest, rest) + (1.0 - scale) * eye for rest in rests]
    gap = gap * gap / (2.0 - gap * gap)
    while True:
        scale = 2.0 / (2.0 - gap * gap)
        gap = gap * gap / (2.0 - gap * gap)
        if gap < 1e-3:
            guesses = [
                scale * (guess + full_dot(rest, guess)) for rest, guess in zip(rests, guesses)
            ]
            break
        both = [
            full_dot(rest, jnp.concatenate([rest, guess], axis=1))
            for rest, guess in zip(rests, guesses)
        ]
        guesses = [scale * (guess + pair[:, size:]) for guess, pair in zip(guesses, both)]
        rests = [scale * pair[:, :size] + (1.0 - scale) * eye for pair in both]
    for _ in range(2):
        errors = [eye - full_dot(block, guess) for block, guess in zip(blocks, guesses)]
        guesses = [guess + dot3(guess, error) for guess, error in zip(guesses, errors)]
    return guesses


SIDES = (-1, 1)
CUTS = 4


def paired_kernel(
    rhs_ref, coords_ref, noise_ref, ids_ref,
    solution_ref, residual_ref,
    info, points_col, ext_row, ext_col, top, low, mats, inv_top, inv_low, pick, put,
    start_res, basis, images, work, work_image, accum, accum_small,
    asked, own_asked, got, tails, back, window, far, mine, slots, coef, far_coef,
    send_sem, recv_sem,
):
    size_x, size_y = lax.axis_size("gx"), lax.axis_size("gy")
    my_x, my_y = lax.axis_index("gx"), lax.axis_index("gy")
    other = 1 - my_y
    points = rhs_ref.shape[0]
    lanes = rhs_ref.shape[1] // 2
    total = 2 * points
    borrowed = ids_ref.shape[1]
    ext = points + borrowed
    row_of_side = {0: 0, -1: 1, 1: 2}

    counter = [0]
    pending = []

    def near(row_off, flip):
        place = {}
        if row_off:
            place["gx"] = lax.rem(my_x + row_off + size_x, size_x)
        if flip:
            place["gy"] = other
        return place

    def send(source, dest, row_off, flip=False):
        index = counter[0]
        counter[0] += 1
        copy = pltpu.make_async_remote_copy(
            src_ref=source,
            dst_ref=dest,
            send_sem=send_sem.at[index],
            recv_sem=recv_sem.at[index],
            device_id=near(row_off, flip),
            device_id_type=MESH,
        )
        copy.start()
        pending.append(copy)
        return copy

    half = lambda which: pl.ds(pl.multiple_of(which * lanes, lanes), lanes)
    column = lambda which: pl.ds(pl.multiple_of(which * points, points), points)

    barrier = pltpu.get_barrier_semaphore()
    for hop in range(1, size_x):
        pl.semaphore_signal(
            barrier, inc=1, device_id={"gx": lax.rem(my_x + hop, size_x)}, device_id_type=MESH
        )
    for row_off in (0, -1, 1):
        pl.semaphore_signal(barrier, inc=1, device_id=near(row_off, True), device_id_type=MESH)

    info[0, my_y] = jnp.concatenate(
        [
            coords_ref[...],
            noise_ref[...],
            jnp.concatenate(
                [
                    ids_ref[...].astype(jnp.float32),
                    jnp.zeros((1, points - borrowed), jnp.float32),
                ],
                axis=1,
            ),
            jnp.zeros((4, points), jnp.float32),
        ],
        axis=0,
    )
    start_res[column(my_y), :] = rhs_ref[:, half(my_y)]
    pl.semaphore_wait(barrier, size_x - 1 + 3)

    facts = []
    for row_off, flip in ((0, True), (-1, False), (1, False), (-1, True), (1, True)):
        dest = info.at[row_of_side[-row_off], my_y]
        facts.append(send(info.at[0, my_y], dest, row_off, flip))
    rhs_move = send(rhs_ref.at[:, half(other)], start_res.at[column(my_y), :], 0, True)
    for fact in facts:
        fact.wait_recv()

    def offset_of(row_of, listed_col):
        return float(3 * row_of * points - (listed_col - 1) * points)

    point_down = lax.broadcasted_iota(jnp.int32, (total, borrowed), 0).astype(jnp.float32)
    point_across = lax.broadcasted_iota(jnp.int32, (borrowed, total), 1).astype(jnp.float32)

    def hot(first, second):
        return jnp.where(first == second, 1.0, 0.0).astype(jnp.bfloat16)

    square_pad = jnp.zeros((borrowed - 8, borrowed), jnp.float32)
    for side in (0, -1, 1):
        place = row_of_side[side]
        for col in range(2):
            facts_here = info[place, col]
            row_ids = facts_here[3:4, :borrowed] - offset_of(1 - side, col)
            slots_here = pl.ds((2 * place + col) * borrowed, borrowed)
            put[:, slots_here] = hot(point_down, row_ids)
            turned = jnp.transpose(
                jnp.concatenate([facts_here[:, :borrowed], square_pad], axis=0)
            )
            pick[slots_here, :] = hot(turned[:, 3:4] - offset_of(1 - side, col), point_across)

    def parts_of(place):
        row = jnp.concatenate([info[place, 0], info[place, 1]], axis=1)
        return jnp.concatenate(
            [part.astype(jnp.float32) for part in split3(row)], axis=0
        ).astype(jnp.bfloat16)

    for col in range(2):
        ids = info[0, col][3:4, :borrowed]
        found = jnp.zeros((24, borrowed), jnp.float32)
        for side in (0, -1, 1):
            place = row_of_side[side]
            found = found + mm(parts_of(place), hot(point_down, ids - offset_of(1 + side, col)))
        found = found[0:8] + found[8:16] + found[16:24]
        row_shift = jnp.where(ids < 3.0 * points, -1.0, jnp.where(ids < 6.0 * points, 0.0, 1.0))
        within = ids - (row_shift + 1.0) * (3.0 * points)
        col_shift = jnp.where(within < points, -1.0, jnp.where(within < 2.0 * points, 0.0, 1.0))
        ext_here = jnp.concatenate(
            [found[0:1] + row_shift, found[1:2] + col_shift, found[2:3], found[3:8]], axis=0
        )
        ext_row[col] = ext_here
        ext_col[col] = jnp.transpose(jnp.concatenate([ext_here, square_pad], axis=0))
        for low_row in range(0, points, borrowed):
            part = info[0, col][:, low_row : low_row + borrowed]
            points_col[pl.ds(col * points + low_row, borrowed), :] = jnp.transpose(
                jnp.concatenate([part, square_pad], axis=0)
            )

    step = 32

    def own_diagonal(start, noise, width):
        here = lax.broadcasted_iota(jnp.int32, (step, width), 0) + start
        across = lax.broadcasted_iota(jnp.int32, (step, width), 1)
        return jnp.where(here == across, noise, 0.0)

    for col in range(2):

        def fill(index, carry, col=col):
            start = index * step
            rows = pl.ds(pl.multiple_of(col * points + start, step), step)
            local = pl.ds(pl.multiple_of(start, step), step)
            mine_x = points_col[rows, 0:1]
            mine_y = points_col[rows, 1:2]
            noise = points_col[rows, 2:3]
            for side in (0, -1, 1):
                place = row_of_side[side]
                for source in range(2):
                    there = info[place, source]
                    block = covariance(
                        mine_x,
                        mine_y,
                        there[0:1] + float(side),
                        there[1:2] + float(source - col),
                    )
                    if side == 0 and source == col:
                        block = block + own_diagonal(start, noise, points)
                        mats[col, local, 0:points] = block
                    cols = slice((2 * place + source) * points, (2 * place + source + 1) * points)
                    top[rows, cols], low[rows, cols] = split(block)
            mats[col, local, points:ext] = covariance(
                mine_x, mine_y, ext_row[col, 0:1], ext_row[col, 1:2]
            )
            return carry

        lax.fori_loop(0, points // step, fill, 0)

        def fill_ext(index, carry, col=col):
            start = index * step
            rows = pl.ds(pl.multiple_of(start, step), step)
            local = pl.ds(pl.multiple_of(points + start, step), step)
            mine_x = ext_col[col, rows, 0:1]
            mine_y = ext_col[col, rows, 1:2]
            noise = ext_col[col, rows, 2:3]
            mats[col, local, 0:points] = covariance(
                mine_x, mine_y, info[0, col, 0:1], info[0, col, 1:2]
            )
            block = covariance(mine_x, mine_y, ext_row[col, 0:1], ext_row[col, 1:2])
            mats[col, local, points:ext] = block + own_diagonal(start, noise, borrowed)
            return carry

        lax.fori_loop(0, borrowed // step, fill_ext, 0)

    def request(turn, value):
        both = wide(value)
        wanted = folded(mm(pick[...], both))
        own_asked[...] = wanted[: 2 * borrowed]
        moves = []
        for index, side in enumerate(SIDES):
            asked[turn, index] = wanted[2 * (index + 1) * borrowed : 2 * (index + 2) * borrowed]
            moves.append(send(asked.at[turn, index], got.at[turn, 1 - index], side))
        return both, moves

    def solve(turn, both, moves):
        for col in range(2):
            part = both[col * points : (col + 1) * points]
            accum_small[col] = mm(inv_top[col, :, :points], part) + mm(
                inv_low[col, :, :points], part
            )
        for move in moves:
            move.wait_recv()
        loaned = []
        for col in range(2):
            rows = slice(col * borrowed, (col + 1) * borrowed)
            loaned.append(wide(own_asked[rows] + got[turn, 0, rows] + got[turn, 1, rows]))
            tails[turn, rows] = folded(
                accum_small[col, points:]
                + mm(inv_top[col, points:, points:], loaned[col])
                + mm(inv_low[col, points:, points:], loaned[col])
            )
        returns = [
            send(tails.at[turn], back.at[turn, 1 - index], side)
            for index, side in enumerate(SIDES)
        ]
        owned = mm(put[:, : 2 * borrowed], wide(tails[turn]))
        for col in range(2):
            rows = slice(col * points, (col + 1) * points)
            basis[turn, rows] = folded(
                accum_small[col, :points]
                + mm(inv_top[col, :points, points:], loaned[col])
                + mm(inv_low[col, :points, points:], loaned[col])
                + owned[rows]
            )
        for move in returns:
            move.wait_recv()
        came = jnp.concatenate([wide(back[turn, 0]), wide(back[turn, 1])], axis=0)
        basis[turn] = basis[turn] + folded(mm(put[:, 2 * borrowed :], came))

    piece = total // CUTS

    def apply(turn):
        moves = []
        for cut in range(CUTS):
            rows = pl.ds(cut * piece, piece)
            for index, side in enumerate(SIDES):
                moves.append(
                    send(basis.at[turn, rows], window.at[turn, 1 - index, rows], side)
                )
        send_far(turn, basis)
        both = wide(basis[turn])
        accum[...] = mm(top[:, :total], both) + mm(low[:, :total], both)
        for cut in range(CUTS):
            for index in range(2):
                moves[2 * cut + index].wait_recv()
            for index in range(2):
                both = wide(window[turn, index, cut * piece : (cut + 1) * piece])
                cols = slice(
                    (index + 1) * total + cut * piece, (index + 1) * total + (cut + 1) * piece
                )
                accum[...] = accum[...] + (mm(top[:, cols], both) + mm(low[:, cols], both))
        images[turn] = folded(accum[...])

    far_moves = []

    def send_far(turn, source):
        index = turn if source is basis else ITERS + turn
        far_moves.append(send(source.at[turn, column(other)], far.at[index], 0, True))

    def begin_sum(turn, rows):
        mine[turn] = jnp.concatenate(rows, axis=0)
        index = counter[0]
        counter[0] += 1
        for hop in range(1, size_x):
            pltpu.make_async_remote_copy(
                src_ref=mine.at[turn],
                dst_ref=slots.at[turn, hop - 1],
                send_sem=send_sem.at[index],
                recv_sem=recv_sem.at[index],
                device_id={"gx": lax.rem(my_x + hop, size_x)},
                device_id_type=MESH,
            ).start()
        return index

    def end_sum(turn, index):
        held = slots.at[turn]
        pltpu.make_async_copy(held, held, recv_sem.at[index]).wait()
        pltpu.make_async_copy(held, held, send_sem.at[index]).wait()
        sums = mine[turn] + jnp.sum(slots[turn], axis=0)
        return sums[0:1], sums[1:2], sums[2:3]

    def inner(first, second):
        return jnp.sum(first * second, axis=0, keepdims=True)

    nothing = jnp.zeros((1, lanes), jnp.float32)

    rhs_move.wait_recv()
    asking = request(0, start_res[...])
    invert_both(mats)
    for col in range(2):
        inv_top[col], inv_low[col] = split(mats[col])
    solve(0, *asking)
    apply(0)
    send_far(0, images)
    summing = begin_sum(
        0, [inner(start_res[...], basis[0]), inner(basis[0], images[0]), nothing]
    )
    asking = request(1, images[0])
    solve(1, *asking)
    apply(1)
    send_far(1, images)
    gamma_0, curve_0, _ = end_sum(0, summing)
    alpha_0 = gamma_0 / curve_0
    work_image[...] = images[0] - alpha_0 * images[1]
    asking = request(2, work_image[...])
    work[...] = basis[0] - alpha_0 * basis[1]
    summing = begin_sum(
        1,
        [
            inner(start_res[...] - alpha_0 * images[0], work[...]),
            inner(work[...], work_image[...]),
            inner(work[...], images[0]),
        ],
    )
    solve(2, *asking)
    gamma_1, curve_1, mixed_1 = end_sum(1, summing)
    beta_1 = gamma_1 / gamma_0
    curve_1 = curve_1 + beta_1 * (2.0 * mixed_1 + beta_1 * curve_0)
    alpha_1 = gamma_1 / curve_1
    apply(2)
    send_far(2, images)
    old_image = work_image[...] + beta_1 * images[0]
    last = work[...] - alpha_1 * (basis[2] + beta_1 * basis[1])
    last_image = work_image[...] - alpha_1 * (images[2] + beta_1 * images[1])
    summing = begin_sum(
        2,
        [
            inner(start_res[...] - alpha_0 * images[0] - alpha_1 * old_image, last),
            inner(last, last_image),
            inner(last, old_image),
        ],
    )
    gamma_2, curve_2, mixed_2 = end_sum(2, summing)
    beta_2 = gamma_2 / gamma_1
    curve_2 = curve_2 + beta_2 * (2.0 * mixed_2 + beta_2 * curve_1)
    alpha_2 = gamma_2 / curve_2
    weights = [
        alpha_0 + alpha_1 * (1.0 + beta_1) + alpha_2 * (1.0 + beta_2 * (1.0 + beta_1)),
        -alpha_1 * alpha_0 - alpha_2 * (alpha_0 + alpha_1 * beta_1 + beta_2 * alpha_0),
        -alpha_2 * alpha_1,
    ]
    coef[...] = jnp.concatenate(weights + [jnp.zeros((5, lanes), jnp.float32)], axis=0)
    told = send(coef, far_coef, 0, True)
    held = column(my_y)
    solution_ref[:, half(my_y)] = (
        weights[0] * basis[0, held] + weights[1] * basis[1, held] + weights[2] * basis[2, held]
    )
    residual_ref[:, half(my_y)] = start_res[held, :] - (
        weights[0] * images[0, held] + weights[1] * images[1, held] + weights[2] * images[2, held]
    )
    for move in far_moves:
        move.wait_recv()
    told.wait_recv()
    weights = [far_coef[index : index + 1] for index in range(ITERS)]
    solution_ref[:, half(other)] = weights[0] * far[0] + weights[1] * far[1] + weights[2] * far[2]
    residual_ref[:, half(other)] = rhs_ref[:, half(other)] - (
        weights[0] * far[3] + weights[1] * far[4] + weights[2] * far[5]
    )
    for move in pending:
        move.wait_send()


def invert_both(mats):
    size = mats.shape[1]
    step = math.gcd(size, 128)
    rows = lax.broadcasted_iota(jnp.int32, (size, step), 0)
    lanes = lax.broadcasted_iota(jnp.int32, (size, step), 1)

    def eliminate(index, carry):
        start = pl.multiple_of(index * step, step)
        here = pl.ds(start, step)
        pivots = pivot_inverses([mats[which, here, here] for which in range(2)])
        inside = jnp.logical_and(rows >= start, rows < start + step)
        for which in range(2):
            column = jnp.where(inside, 0.0, mats[which, :, here])
            mats[which, :, here] = jnp.where(rows - start == lanes, 1.0, 0.0)
            row = full_dot(pivots[which], mats[which, here, :])
            mats[which] = mats[which] - full_dot(column, row)
            mats[which, here, :] = row
        return carry

    lax.fori_loop(0, size // step, eliminate, 0)


def paired_solve(right_side, coords, noise, intersect):
    points, width = right_side.shape
    size_x = lax.axis_size("gx")
    borrowed = intersect.shape[1]
    lanes, total, ext = width // 2, 2 * points, points + borrowed
    moves = 5 + 1 + ITERS * (2 + 2 + 2 * CUTS + 2 + 1) + 1
    out = jax.ShapeDtypeStruct(right_side.shape, jnp.float32)
    f32 = lambda *shape: pltpu.VMEM(shape, jnp.float32)
    b16 = lambda *shape: pltpu.VMEM(shape, jnp.bfloat16)
    return pl.pallas_call(
        paired_kernel,
        out_shape=(out, out),
        in_specs=[VMEM] * 4,
        out_specs=(VMEM, VMEM),
        scratch_shapes=[
            f32(3, 2, 8, points),
            f32(total, borrowed),
            f32(2, 8, borrowed),
            f32(2, borrowed, borrowed),
            b16(total, 3 * total),
            b16(total, 3 * total),
            f32(2, ext, ext),
            b16(2, ext, ext),
            b16(2, ext, ext),
            b16(6 * borrowed, total),
            b16(total, 6 * borrowed),
            f32(total, lanes),
            f32(ITERS, total, lanes),
            f32(ITERS, total, lanes),
            f32(total, lanes),
            f32(total, lanes),
            f32(total, 2 * lanes),
            f32(2, ext, 2 * lanes),
            f32(ITERS, 2, 2 * borrowed, lanes),
            f32(2 * borrowed, lanes),
            f32(ITERS, 2, 2 * borrowed, lanes),
            f32(ITERS, 2 * borrowed, lanes),
            f32(ITERS, 2, 2 * borrowed, lanes),
            f32(ITERS, 2, total, lanes),
            f32(2 * ITERS, points, lanes),
            f32(ITERS, 3, lanes),
            f32(ITERS, size_x - 1, 3, lanes),
            f32(8, lanes),
            f32(8, lanes),
            pltpu.SemaphoreType.DMA((moves,)),
            pltpu.SemaphoreType.DMA((moves,)),
        ],
        compiler_params=pltpu.CompilerParams(
            collective_id=0, has_side_effects=True, vmem_limit_bytes=58 * 1024 * 1024
        ),
    )(right_side, coords, noise, intersect)


def paired_shards(right_side, coords, noise, intersect):
    points, width = right_side.shape[2:]
    answer, residual = paired_solve(
        right_side.reshape(points, width),
        coords.reshape(2, points),
        noise.reshape(1, points),
        intersect.reshape(1, intersect.shape[2]),
    )
    return answer.reshape(right_side.shape), residual.reshape(right_side.shape)


def solution(mesh):
    placed = (
        P("gx", "gy", None, None),
        P("gx", "gy", None, None),
        P("gx", "gy", None),
        P("gx", "gy", None),
    )
    return jax.shard_map(
        paired_shards if mesh.shape["gy"] == 2 else shards,
        mesh=mesh,
        in_specs=placed,
        out_specs=(P("gx", "gy", None, None), P("gx", "gy", None, None)),
        check_vma=False,
    )
```

```python
import functools
import math

import jax
import jax.numpy as jnp
from jax import lax
from jax.experimental import pallas as pl
from jax.experimental.pallas import tpu as pltpu
from jax.sharding import PartitionSpec as P

ITERS = 3


RANGE_LEN = 0.25
ROOT_THREE = math.sqrt(3.0)
HIGH = lax.Precision.HIGHEST


def shifted(value, axis, by):
    count = lax.axis_size(axis)
    return lax.ppermute(value, axis, [(i, (i + by) % count) for i in range(count)])


def passed_along(block, axis, distance):
    devices = range(lax.axis_size(axis))
    route = [(i - distance, i) for i in devices if i - distance in devices]
    return lax.ppermute(block, axis, route)


def kernel_block(rows_pos, cols_pos):
    delta_x = rows_pos[0][:, None] - cols_pos[0][None, :]
    delta_y = rows_pos[1][:, None] - cols_pos[1][None, :]
    distance = jnp.sqrt(delta_x * delta_x + delta_y * delta_y)
    scaled = ROOT_THREE / RANGE_LEN * distance
    clipped = jnp.minimum(distance, 1.0)
    taper_val = jnp.square(jnp.square(1.0 - clipped)) * (4.0 * clipped + 1.0)
    return (1.0 + scaled) * jnp.exp(-scaled) * taper_val


def window_values(values):
    beside = {}
    for step_by in (1, -1):
        beside[step_by] = shifted(values, "gx", step_by)
    column = jnp.stack([beside[1], values, beside[-1]])
    across = {}
    for step_by in (1, -1):
        across[step_by] = passed_along(column, "gy", step_by)
    return [across[1], column, across[-1]]


CHUNKS = 4
MESH = pl.DeviceIdType.MESH
NOISE_MIN = 0.25
VMEM = pl.BlockSpec(memory_space=pltpu.VMEM)


def split(value):
    top = value.astype(jnp.bfloat16)
    return top, (value - top.astype(jnp.float32)).astype(jnp.bfloat16)


def dot3(left, right):
    left_top, left_low = split(left)
    right_top, right_low = split(right)
    return jnp.dot(
        jnp.concatenate([left_top, left_top, left_low], axis=1),
        jnp.concatenate([right_top, right_low, right_top], axis=0),
        preferred_element_type=jnp.float32,
    )


def dot6(left, right):
    return jnp.dot(left, right, precision=HIGH, preferred_element_type=jnp.float32)


def block_inverse(block):
    size = block.shape[0]
    low, high = NOISE_MIN * 0.97, (size + 1.0) * 1.01
    eye = (
        lax.broadcasted_iota(jnp.int32, block.shape, 0)
        == lax.broadcasted_iota(jnp.int32, block.shape, 1)
    ).astype(jnp.float32)
    first = 2.0 / (low + high)
    gap = 1.0 - first * low
    scale = 2.0 / (2.0 - gap * gap)
    guess = (2.0 * first * scale) * eye - (first * first * scale) * block
    gap = gap * gap / (2.0 - gap * gap)
    while gap > 1e-3:
        scale = 2.0 / (2.0 - gap * gap)
        rest = 2.0 * eye - dot3(block, guess)
        guess = scale * dot3(guess, rest)
        gap = gap * gap / (2.0 - gap * gap)
    for _ in range(2):
        guess = guess + dot3(guess, eye - dot6(block, guess))
    return guess


def invert(matrix_ref, out_ref):
    size = matrix_ref.shape[0]
    step = math.gcd(size, 128)
    out_ref[...] = matrix_ref[...]
    for start in range(0, size, step):
        here = slice(start, start + step)
        pivot = block_inverse(out_ref[here, here])
        column = out_ref[:, here]
        row = dot6(pivot, out_ref[here, :])
        for low in range(0, size, step):
            if low != start:
                part = slice(low, low + step)
                out_ref[part, :] = out_ref[part, :] - dot6(column[part], row)
                out_ref[part, here] = -dot6(column[part], pivot)
        out_ref[here, :] = row
        out_ref[here, here] = pivot


def columns_of(count):
    return () if count == 1 else (1,) if count == 2 else (-1, 1)


def opposite(col_off, count):
    return col_off if count == 2 else -col_off


def offsets_of(count):
    near = [(-1, 0), (1, 0)]
    for col_off in columns_of(count):
        near += [(0, col_off), (-1, col_off), (1, col_off)]
    return near


def cg_kernel(
    rhs_ref, window_ref, matrix_ref, pick_ref, put_ref,
    solution_ref, residual_ref,
    top_ref, low_ref, inverse, inv_top_ref, inv_low_ref, asked, got, tail, back, precond, window, direction, image, mine, slots_y, slots_x,
    send_sem, recv_sem,
):
    size_x, size_y = lax.axis_size("gx"), lax.axis_size("gy")
    my_x, my_y = lax.axis_index("gx"), lax.axis_index("gy")
    near = offsets_of(size_y)
    points = rhs_ref.shape[0]
    borrowed = tail.shape[0]
    half = points // CHUNKS

    def inside(col_off):
        if col_off == 0 or size_y == 2:
            return None
        return my_y > 0 if col_off < 0 else my_y < size_y - 1

    def guarded(condition, action):
        if condition is None:
            action()
        else:
            pl.when(condition)(action)

    def target(row_off, col_off):
        place = {}
        if row_off:
            place["gx"] = lax.rem(my_x + row_off + size_x, size_x)
        if col_off:
            place["gy"] = 1 - my_y if size_y == 2 else my_y + col_off
        return place

    counter = [0]

    class Move:
        def __init__(self, source, dest, row_off, col_off):
            index = counter[0]
            counter[0] += 1
            self.copy = pltpu.make_async_remote_copy(
                src_ref=source,
                dst_ref=dest,
                send_sem=send_sem.at[index],
                recv_sem=recv_sem.at[index],
                device_id=target(row_off, col_off),
                device_id_type=MESH,
            )
            self.out = inside(col_off)
            self.into = inside(-col_off)

        def start(self):
            guarded(self.out, self.copy.start)

        def sent(self):
            guarded(self.out, self.copy.wait_send)

        def landed(self):
            guarded(self.into, self.copy.wait_recv)

    def slot(row_off, col_off):
        return near.index((-row_off, opposite(col_off, size_y)))

    barrier = pltpu.get_barrier_semaphore()
    greeted = 0
    for axis, here, count in (("gx", my_x, size_x), ("gy", my_y, size_y)):
        for hop in range(1, count):
            pl.semaphore_signal(
                barrier, inc=1, device_id={axis: lax.rem(here + hop, count)}, device_id_type=MESH
            )
            greeted += 1
    for row_off, col_off in near:
        if row_off and col_off:

            def greet(row_off=row_off, col_off=col_off):
                pl.semaphore_signal(
                    barrier, inc=1, device_id=target(row_off, col_off), device_id_type=MESH
                )

            guarded(inside(col_off), greet)
            there = inside(col_off)
            greeted = greeted + (1 if there is None else jnp.where(there, 1, 0))

    for col_off in columns_of(size_y):
        there = inside(col_off)
        if there is not None:

            def clear(col_off=col_off):
                for index, (_, col) in enumerate(near):
                    if col == col_off:
                        for iteration in range(ITERS):
                            got[iteration, index] = jnp.zeros(tail.shape, jnp.float32)
                            back[iteration, index] = jnp.zeros(tail.shape, jnp.float32)
                            window[iteration, index] = jnp.zeros(rhs_ref.shape, jnp.float32)

            pl.when(jnp.logical_not(there))(clear)

    def exact_dot(ones, value):
        top, low = split(value)
        return jnp.dot(ones, top, preferred_element_type=jnp.float32) + jnp.dot(
            ones, low, preferred_element_type=jnp.float32
        )

    def dot_parts(left_top, left_low, right):
        right_top, right_low = split(right)
        return (
            jnp.dot(left_top, right_top, preferred_element_type=jnp.float32)
            + jnp.dot(left_top, right_low, preferred_element_type=jnp.float32)
            + jnp.dot(left_low, right_top, preferred_element_type=jnp.float32)
        )

    def window_part(block, value):
        cols = slice(block * points, (block + 1) * points)
        return dot_parts(top_ref[:, cols], low_ref[:, cols], value)

    def total(iteration):
        for stage, (axis, here, count, slots) in enumerate(
            (("gy", my_y, size_y, slots_y), ("gx", my_x, size_x, slots_x))
        ):
            index = counter[0]
            counter[0] += 1
            for hop in range(1, count):
                pltpu.make_async_remote_copy(
                    src_ref=mine.at[iteration, stage],
                    dst_ref=slots.at[iteration, hop - 1],
                    send_sem=send_sem.at[index],
                    recv_sem=recv_sem.at[index],
                    device_id={axis: lax.rem(here + hop, count)},
                    device_id_type=MESH,
                ).start()
            so_far = mine[iteration, stage]
            if count > 1:
                held = slots.at[iteration]
                pltpu.make_async_copy(held, held, recv_sem.at[index]).wait()
                so_far = so_far + jnp.sum(slots[iteration], axis=0)
                pltpu.make_async_copy(held, held, send_sem.at[index]).wait()
            mine[iteration, stage + 1] = so_far
        return mine[iteration, 2]

    residual_ref[...] = rhs_ref[...]
    wait_entry = [True]
    inner_old = denominator = None
    for iteration in range(ITERS):
        requests = exact_dot(pick_ref[...], residual_ref[...])
        for index in range(len(near)):
            asked[index] = requests[index * borrowed : (index + 1) * borrowed]
        if wait_entry[0]:
            pl.semaphore_wait(barrier, greeted)
            wait_entry[0] = False
        moves = [
            Move(asked.at[index], got.at[iteration, slot(*offset)], *offset)
            for index, offset in enumerate(near)
        ]
        for move in moves:
            move.start()
        if iteration == 0:
            invert(matrix_ref, inverse)
            inv_top_ref[...], inv_low_ref[...] = split(inverse[...])
            top_ref[...], low_ref[...] = split(window_ref[...])
        solved = dot_parts(
            inv_top_ref[:, :points], inv_low_ref[:, :points], residual_ref[...]
        )
        for move in moves:
            move.landed()
        gathered = jnp.sum(got[iteration], axis=0)
        solved = solved + dot_parts(inv_top_ref[:, points:], inv_low_ref[:, points:], gathered)
        tail[...] = solved[points:]
        precond[...] = solved[:points]
        returns = [Move(tail, back.at[iteration, slot(*offset)], *offset) for offset in near]
        for move in returns:
            move.start()
        for move in moves:
            move.sent()
        for move in returns:
            move.landed()
        returned = back[iteration].reshape(len(near) * borrowed, tail.shape[1])
        precond[...] = precond[...] + exact_dot(put_ref[...], returned)
        for move in returns:
            move.sent()

        sides, relays = [], []
        for chunk in range(CHUNKS):
            rows = pl.ds(chunk * half, half)
            for col_off in columns_of(size_y):
                index = slot(0, col_off)
                sides.append(
                    Move(precond.at[rows], window.at[iteration, index, rows], 0, col_off)
                )
                sides[-1].start()
        beside = [
            Move(precond, window.at[iteration, slot(row_off, 0)], row_off, 0)
            for row_off in (-1, 1)
        ]
        for move in beside:
            move.start()
        result = window_part(len(near), precond[...])
        place = 0
        for chunk in range(CHUNKS):
            rows = pl.ds(chunk * half, half)
            for col_off in columns_of(size_y):
                sides[place].landed()
                place += 1
                source = near.index((0, opposite(col_off, size_y)))
                for row_off in (-1, 1):
                    index = near.index((-row_off, opposite(col_off, size_y)))
                    move = Move(
                        window.at[iteration, source, rows],
                        window.at[iteration, index, rows],
                        row_off,
                        0,
                    )
                    there = inside(-col_off)
                    move.out = move.into = there
                    relays.append(move)
                    move.start()
        for index, (row_off, col_off) in enumerate(near):
            if row_off == 0:
                result = result + window_part(index, window[iteration, index])
        for move in beside:
            move.landed()
        for index, (row_off, col_off) in enumerate(near):
            if row_off and col_off == 0:
                result = result + window_part(index, window[iteration, index])
        for move in relays:
            move.landed()
        for index, (row_off, col_off) in enumerate(near):
            if row_off and col_off:
                result = result + window_part(index, window[iteration, index])
        fresh = precond[...]
        mine[iteration, 0, 0:1] = jnp.sum(residual_ref[...] * fresh, axis=0, keepdims=True)
        mine[iteration, 0, 1:2] = jnp.sum(fresh * result, axis=0, keepdims=True)
        if iteration:
            mine[iteration, 0, 2:3] = jnp.sum(fresh * image[...], axis=0, keepdims=True)
        else:
            mine[iteration, 0, 2:3] = jnp.zeros((1, fresh.shape[1]), jnp.float32)
        sums = total(iteration)
        for move in sides + beside + relays:
            move.sent()
        inner, curved, mixed = sums[0:1], sums[1:2], sums[2:3]
        if iteration:
            ratio = inner / inner_old
            denominator = curved + ratio * (2.0 * mixed + ratio * denominator)
            direction[...] = fresh + ratio * direction[...]
            image[...] = result + ratio * image[...]
        else:
            denominator = curved
            direction[...] = fresh
            image[...] = result
        inner_old = inner
        step_size = inner / denominator
        moved = step_size * direction[...]
        solution_ref[...] = solution_ref[...] + moved if iteration else moved
        residual_ref[...] = residual_ref[...] - step_size * image[...]


def conjugate_gradients(right_side, window_matrix, matrix, pick):
    near = offsets_of(lax.axis_size("gy"))
    points, width = right_side.shape
    borrowed = matrix.shape[0] - points
    size_x, size_y = lax.axis_size("gx"), lax.axis_size("gy")
    sides = len(columns_of(size_y))
    moves = ITERS * (2 * len(near) + 2 + 3 * CHUNKS * sides + 2)
    out = jax.ShapeDtypeStruct(right_side.shape, jnp.float32)
    block = pltpu.VMEM((points, width), jnp.float32)
    small = (len(near), borrowed, width)
    return pl.pallas_call(
        cg_kernel,
        out_shape=(out, out),
        in_specs=[VMEM] * 5,
        out_specs=(VMEM, VMEM),
        scratch_shapes=[
            pltpu.VMEM(window_matrix.shape, jnp.bfloat16),
            pltpu.VMEM(window_matrix.shape, jnp.bfloat16),
            pltpu.VMEM(matrix.shape, jnp.float32),
            pltpu.VMEM(matrix.shape, jnp.bfloat16),
            pltpu.VMEM(matrix.shape, jnp.bfloat16),
            pltpu.VMEM(small, jnp.float32),
            pltpu.VMEM((ITERS,) + small, jnp.float32),
            pltpu.VMEM((borrowed, width), jnp.float32),
            pltpu.VMEM((ITERS,) + small, jnp.float32),
            block,
            pltpu.VMEM((ITERS, len(near), points, width), jnp.float32),
            block,
            block,
            pltpu.VMEM((ITERS, 3, 3, width), jnp.float32),
            pltpu.VMEM((ITERS, max(size_y - 1, 1), 3, width), jnp.float32),
            pltpu.VMEM((ITERS, max(size_x - 1, 1), 3, width), jnp.float32),
            pltpu.SemaphoreType.DMA((moves,)),
            pltpu.SemaphoreType.DMA((moves,)),
        ],
        compiler_params=pltpu.CompilerParams(
            collective_id=0, has_side_effects=True, vmem_limit_bytes=56 * 1024 * 1024
        ),
    )(right_side, window_matrix, matrix, pick, pick.T)


def shards(right_side, coords, noise, intersect):
    points = right_side.shape[2]
    rhs_count = right_side.shape[3]
    intersect_len = intersect.shape[2]
    ext_len = points + intersect_len
    own_pos = coords.reshape(2, points)
    own_noise = noise.reshape(points)
    listed = jnp.pad(intersect.reshape(intersect_len), (0, points - intersect_len))
    point_info = jnp.concatenate(
        [own_pos, own_noise[None, :], listed.astype(jnp.float32)[None, :]], axis=0
    )
    info_cols = window_values(point_info)
    intersect_ids = intersect.reshape(intersect_len)
    block_id = intersect_ids // points
    row_in = intersect_ids % points
    row_of = block_id // 3
    col_of = block_id % 3
    local_id = row_of * points + row_in
    picked_info = [
        jnp.take(
            jnp.transpose(info_cols[col_off], (1, 0, 2)).reshape(4, 3 * points), local_id, axis=1
        )
        for col_off in range(3)
    ]
    chosen = jnp.where(
        col_of[None, :] == 0,
        picked_info[0],
        jnp.where(col_of[None, :] == 1, picked_info[1], picked_info[2]),
    )
    ov_pos = jnp.stack(
        [chosen[0] + (row_of - 1).astype(jnp.float32), chosen[1] + (col_of - 1).astype(jnp.float32)]
    )
    ext_pos = jnp.concatenate([own_pos, ov_pos], axis=1)
    ext_noise = jnp.concatenate([own_noise, chosen[2]])
    local_matrix = kernel_block(ext_pos, ext_pos) + jnp.diag(ext_noise)
    count = lax.axis_size("gy")
    point_iota = jnp.arange(points, dtype=jnp.int32)[None, :]
    blocks, picks = [], []
    for row_off, col_off in offsets_of(count) + [(0, 0)]:
        step = col_off
        info = info_cols[col_off + 1][row_off + 1]
        if col_off and count == 2:
            first = lax.axis_index("gy") == 0
            step = jnp.where(first, 1, -1)
            info = jnp.where(first, info, info_cols[0][row_off + 1])
        shift = jnp.asarray(step, jnp.float32)
        blocks.append(
            kernel_block(own_pos, jnp.stack([info[0] + float(row_off), info[1] + shift]))
        )
        if row_off or col_off:
            ids = info[3, :intersect_len].astype(jnp.int32)
            own_rows = ids - (3 * (1 - row_off) + (1 - step)) * points
            picks.append((own_rows[:, None] == point_iota).astype(jnp.bfloat16))
    blocks[-1] = blocks[-1] + jnp.diag(own_noise)
    answer, residual = conjugate_gradients(
        right_side.reshape(points, rhs_count),
        jnp.concatenate(blocks, axis=1),
        local_matrix,
        jnp.concatenate(picks, axis=0),
    )
    return (answer.reshape(1, 1, points, rhs_count), residual.reshape(1, 1, points, rhs_count))


def split3(value):
    top = value.astype(jnp.bfloat16)
    rest = value - top.astype(jnp.float32)
    mid = rest.astype(jnp.bfloat16)
    return top, mid, (rest - mid.astype(jnp.float32)).astype(jnp.bfloat16)


def full_dot(left, right):
    lt, lm, ll = split3(left)
    rt, rm, rl = split3(right)
    return jnp.dot(
        jnp.concatenate([lt, lt, lm, lm, lt, ll], axis=1),
        jnp.concatenate([rt, rm, rt, rm, rl, rt], axis=0),
        preferred_element_type=jnp.float32,
    )


def wide(value):
    return jnp.concatenate(split(value), axis=1)


def folded(value):
    lanes = value.shape[1] // 2
    return value[:, :lanes] + value[:, lanes:]


def mm(left, right):
    return jnp.dot(left, right, preferred_element_type=jnp.float32)


def covariance(rows_x, rows_y, cols_x, cols_y):
    delta_x = rows_x - cols_x
    delta_y = rows_y - cols_y
    square = delta_x * delta_x + delta_y * delta_y
    distance = square * lax.rsqrt(jnp.maximum(square, 1e-30))
    scaled = ROOT_THREE / RANGE_LEN * distance
    rest = 1.0 - jnp.minimum(distance, 1.0)
    rest = rest * rest
    taper = rest * rest * (4.0 * jnp.minimum(distance, 1.0) + 1.0)
    return (1.0 + scaled) * jnp.exp(-scaled) * taper


def pivot_inverses(blocks, between=lambda: None):
    size = blocks[0].shape[0]
    low, high = NOISE_MIN * 0.97, (size + 1.0) * 1.01
    eye = (
        lax.broadcasted_iota(jnp.int32, blocks[0].shape, 0)
        == lax.broadcasted_iota(jnp.int32, blocks[0].shape, 1)
    ).astype(jnp.float32)
    first = 2.0 / (low + high)
    gap = 1.0 - first * low
    rests = [eye - first * block for block in blocks]
    scale = 2.0 / (2.0 - gap * gap)
    guesses = [(scale * first) * (eye + rest) for rest in rests]
    rests = [scale * full_dot(rest, rest) + (1.0 - scale) * eye for rest in rests]
    between()
    gap = gap * gap / (2.0 - gap * gap)
    while True:
        scale = 2.0 / (2.0 - gap * gap)
        gap = gap * gap / (2.0 - gap * gap)
        if gap < 1e-3:
            guesses = [
                scale * (guess + full_dot(rest, guess)) for rest, guess in zip(rests, guesses)
            ]
            between()
            break
        both = [
            full_dot(rest, jnp.concatenate([rest, guess], axis=1))
            for rest, guess in zip(rests, guesses)
        ]
        guesses = [scale * (guess + pair[:, size:]) for guess, pair in zip(guesses, both)]
        rests = [scale * pair[:, :size] + (1.0 - scale) * eye for pair in both]
        between()
    for _ in range(2):
        errors = [eye - full_dot(block, guess) for block, guess in zip(blocks, guesses)]
        between()
        guesses = [guess + dot3(guess, error) for guess, error in zip(guesses, errors)]
        between()
    return guesses


SIDES = (-1, 1)
CUTS = 4


def paired_kernel(
    rhs_ref, coords_ref, noise_ref, ids_ref,
    solution_ref, residual_ref,
    info, points_col, ext_row, ext_col, top, low, mats, inv_top, inv_low, pick, put,
    start_res, basis, images, work, work_image, last, old_image, accum, accum_small,
    asked, own_asked, got, tails, back, window, far, mine, slots, pivots, crossing,
    send_sem, recv_sem,
):
    size_x, size_y = lax.axis_size("gx"), lax.axis_size("gy")
    my_x, my_y = lax.axis_index("gx"), lax.axis_index("gy")
    other = 1 - my_y
    points = rhs_ref.shape[0]
    lanes = rhs_ref.shape[1] // 2
    total = 2 * points
    borrowed = ids_ref.shape[1]
    ext = points + borrowed
    row_of_side = {0: 0, -1: 1, 1: 2}

    counter = [0]
    pending = []

    def near(row_off, flip):
        place = {}
        if row_off:
            place["gx"] = lax.rem(my_x + row_off + size_x, size_x)
        if flip:
            place["gy"] = other
        return place

    def send(source, dest, row_off, flip=False):
        index = counter[0]
        counter[0] += 1
        copy = pltpu.make_async_remote_copy(
            src_ref=source,
            dst_ref=dest,
            send_sem=send_sem.at[index],
            recv_sem=recv_sem.at[index],
            device_id=near(row_off, flip),
            device_id_type=MESH,
        )
        copy.start()
        pending.append(copy)
        return copy

    half = lambda which: pl.ds(pl.multiple_of(which * lanes, lanes), lanes)
    column = lambda which: pl.ds(pl.multiple_of(which * points, points), points)

    barrier = pltpu.get_barrier_semaphore()
    peers = [(hop, False) for hop in range(1, size_x)] + [(hop, True) for hop in range(size_x)]
    for hop, flip in peers:
        pl.semaphore_signal(barrier, inc=1, device_id=near(hop, flip), device_id_type=MESH)

    info[0, my_y] = jnp.concatenate(
        [
            coords_ref[...],
            noise_ref[...],
            jnp.concatenate(
                [
                    ids_ref[...].astype(jnp.float32),
                    jnp.zeros((1, points - borrowed), jnp.float32),
                ],
                axis=1,
            ),
            jnp.zeros((4, points), jnp.float32),
        ],
        axis=0,
    )
    start_res[column(my_y), :] = rhs_ref[:, half(my_y)]
    pl.semaphore_wait(barrier, len(peers))

    facts = []
    for row_off, flip in ((0, True), (-1, False), (1, False), (-1, True), (1, True)):
        dest = info.at[row_of_side[-row_off], my_y]
        facts.append(send(info.at[0, my_y], dest, row_off, flip))
    rhs_move = send(rhs_ref.at[:, half(other)], start_res.at[column(my_y), :], 0, True)
    for fact in facts:
        fact.wait_recv()

    def offset_of(row_of, listed_col):
        return float(3 * row_of * points - (listed_col - 1) * points)

    point_down = lax.broadcasted_iota(jnp.int32, (total, borrowed), 0).astype(jnp.float32)
    point_across = lax.broadcasted_iota(jnp.int32, (borrowed, total), 1).astype(jnp.float32)

    def hot(first, second):
        return jnp.where(first == second, 1.0, 0.0).astype(jnp.bfloat16)

    square_pad = jnp.zeros((borrowed - 8, borrowed), jnp.float32)
    for side in (0, -1, 1):
        place = row_of_side[side]
        for col in range(2):
            facts_here = info[place, col]
            row_ids = facts_here[3:4, :borrowed] - offset_of(1 - side, col)
            slots_here = pl.ds((2 * place + col) * borrowed, borrowed)
            put[:, slots_here] = hot(point_down, row_ids)
            turned = jnp.transpose(
                jnp.concatenate([facts_here[:, :borrowed], square_pad], axis=0)
            )
            pick[slots_here, :] = hot(turned[:, 3:4] - offset_of(1 - side, col), point_across)

    def parts_of(place):
        row = jnp.concatenate([info[place, 0], info[place, 1]], axis=1)
        return jnp.concatenate(
            [part.astype(jnp.float32) for part in split3(row)], axis=0
        ).astype(jnp.bfloat16)

    for col in range(2):
        ids = info[0, col][3:4, :borrowed]
        found = jnp.zeros((24, borrowed), jnp.float32)
        for side in (0, -1, 1):
            place = row_of_side[side]
            found = found + mm(parts_of(place), hot(point_down, ids - offset_of(1 + side, col)))
        found = found[0:8] + found[8:16] + found[16:24]
        row_shift = jnp.where(ids < 3.0 * points, -1.0, jnp.where(ids < 6.0 * points, 0.0, 1.0))
        within = ids - (row_shift + 1.0) * (3.0 * points)
        col_shift = jnp.where(within < points, -1.0, jnp.where(within < 2.0 * points, 0.0, 1.0))
        ext_here = jnp.concatenate(
            [found[0:1] + row_shift, found[1:2] + col_shift, found[2:3], found[3:8]], axis=0
        )
        ext_row[col] = ext_here
        ext_col[col] = jnp.transpose(jnp.concatenate([ext_here, square_pad], axis=0))
        for low_row in range(0, points, borrowed):
            part = info[0, col][:, low_row : low_row + borrowed]
            points_col[pl.ds(col * points + low_row, borrowed), :] = jnp.transpose(
                jnp.concatenate([part, square_pad], axis=0)
            )

    step = 32

    def own_diagonal(start, noise, width):
        here = lax.broadcasted_iota(jnp.int32, (step, width), 0) + start
        across = lax.broadcasted_iota(jnp.int32, (step, width), 1)
        return jnp.where(here == across, noise, 0.0)

    def block_of(rows, col, side, source):
        there = info[row_of_side[side], source]
        return covariance(
            points_col[rows, 0:1],
            points_col[rows, 1:2],
            there[0:1] + float(side),
            there[1:2] + float(source - col),
        )

    def cols_of(side, source):
        at = (2 * row_of_side[side] + source) * points
        return slice(at, at + points)

    def fill(pairs, rows_step):
        for col in range(2):

            def some(index, carry, col=col):
                start = pl.multiple_of(col * points + index * rows_step, rows_step)
                rows = pl.ds(start, rows_step)
                for side, source in pairs(col):
                    cols = cols_of(side, source)
                    top[rows, cols], low[rows, cols] = split(block_of(rows, col, side, source))
                return carry

            lax.fori_loop(0, points // rows_step, some, 0)

    def fill_cross():
        fill(lambda col: [(0, 1 - col)], 32)

    def fill_sides():
        fill(lambda col: [(side, source) for side in SIDES for source in range(2)], 32)

    for col in range(2):

        def fill_own(index, carry, col=col):
            start = index * step
            rows = pl.ds(pl.multiple_of(col * points + start, step), step)
            local = pl.ds(pl.multiple_of(start, step), step)
            block = block_of(rows, col, 0, col)
            block = block + own_diagonal(start, points_col[rows, 2:3], points)
            mats[col, local, 0:points] = block
            cols = cols_of(0, col)
            top[rows, cols], low[rows, cols] = split(block)
            mats[col, local, points:ext] = covariance(
                points_col[rows, 0:1], points_col[rows, 1:2],
                ext_row[col, 0:1], ext_row[col, 1:2],
            )
            return carry

        lax.fori_loop(0, points // step, fill_own, 0)

        def fill_ext(index, carry, col=col):
            start = index * step
            rows = pl.ds(pl.multiple_of(start, step), step)
            local = pl.ds(pl.multiple_of(points + start, step), step)
            mine_x = ext_col[col, rows, 0:1]
            mine_y = ext_col[col, rows, 1:2]
            noise = ext_col[col, rows, 2:3]
            mats[col, local, 0:points] = covariance(
                mine_x, mine_y, info[0, col, 0:1], info[0, col, 1:2]
            )
            block = covariance(mine_x, mine_y, ext_row[col, 0:1], ext_row[col, 1:2])
            mats[col, local, points:ext] = block + own_diagonal(start, noise, borrowed)
            return carry

        lax.fori_loop(0, borrowed // step, fill_ext, 0)

    def joined(first, second, both):
        return mm(
            jnp.concatenate([first, second], axis=1), jnp.concatenate([both, both], axis=0)
        )

    def request(turn, value):
        both = wide(value)
        wanted = folded(mm(pick[...], both))
        own_asked[...] = wanted[: 2 * borrowed]
        moves = []
        for index, side in enumerate(SIDES):
            asked[turn, index] = wanted[2 * (index + 1) * borrowed : 2 * (index + 2) * borrowed]
            moves.append(send(asked.at[turn, index], got.at[turn, 1 - index], side))
        return both, moves

    def solve(turn, both, moves, meanwhile=lambda: None):
        for col in range(2):
            part = both[col * points : (col + 1) * points]
            accum_small[col] = joined(inv_top[col, :, :points], inv_low[col, :, :points], part)
        for move in moves:
            move.wait_recv()
        loaned = []
        for col in range(2):
            rows = slice(col * borrowed, (col + 1) * borrowed)
            loaned.append(wide(own_asked[rows] + got[turn, 0, rows] + got[turn, 1, rows]))
            tails[turn, rows] = folded(
                accum_small[col, points:]
                + joined(inv_top[col, points:, points:], inv_low[col, points:, points:], loaned[col])
            )
        returns = [
            send(tails.at[turn], back.at[turn, 1 - index], side)
            for index, side in enumerate(SIDES)
        ]
        owned = mm(put[:, : 2 * borrowed], wide(tails[turn]))
        for col in range(2):
            rows = slice(col * points, (col + 1) * points)
            basis[turn, rows] = folded(
                accum_small[col, :points]
                + joined(inv_top[col, :points, points:], inv_low[col, :points, points:], loaned[col])
                + owned[rows]
            )
        meanwhile()
        for move in returns:
            move.wait_recv()
        came = jnp.concatenate([wide(back[turn, 0]), wide(back[turn, 1])], axis=0)
        basis[turn] = basis[turn] + folded(mm(put[:, 2 * borrowed :], came))

    piece = total // CUTS
    close = 1 - lax.rem(my_x, 2)

    def apply(turn, meanwhile=lambda: None):
        first = counter[0]
        for cut in range(CUTS):
            rows = pl.ds(cut * piece, piece)
            for index, side in enumerate(SIDES):
                send(basis.at[turn, rows], window.at[turn, 1 - index, rows], side)
        send_far(turn, basis)

        def landed(cut, index):
            place = window.at[turn, index, pl.ds(cut * piece, piece)]
            semaphore = recv_sem.at[first + 2 * cut + 1 - index]
            pltpu.make_async_copy(place, place, semaphore).wait()

        accum[...] = joined(top[:, :total], low[:, :total], wide(basis[turn]))
        meanwhile()
        for cut in range(CUTS):
            landed(cut, close)
        cols = pl.ds(pl.multiple_of((close + 1) * total, total), total)
        accum[...] = accum[...] + joined(top[:, cols], low[:, cols], wide(window[turn, close]))
        for cut in range(CUTS):
            landed(cut, 1 - close)
            both = wide(window[turn, 1 - close, cut * piece : (cut + 1) * piece])
            cols = pl.ds(pl.multiple_of((2 - close) * total + cut * piece, piece), piece)
            accum[...] = accum[...] + joined(top[:, cols], low[:, cols], both)
        images[turn] = folded(accum[...])

    far_moves = []

    def send_far(turn, source):
        index = turn if source is basis else ITERS + turn
        far_moves.append(send(source.at[turn, column(other)], far.at[index], 0, True))

    def begin_sum(turn, rows):
        mine[turn] = jnp.concatenate(rows, axis=0)
        index = counter[0]
        counter[0] += 1
        for place, (hop, flip) in enumerate(peers):
            pltpu.make_async_remote_copy(
                src_ref=mine.at[turn],
                dst_ref=slots.at[turn, place],
                send_sem=send_sem.at[index],
                recv_sem=recv_sem.at[index],
                device_id=near(hop, flip),
                device_id_type=MESH,
            ).start()
        return index

    def end_sum(turn, index):
        held = slots.at[turn]
        pltpu.make_async_copy(held, held, recv_sem.at[index]).wait()
        pltpu.make_async_copy(held, held, send_sem.at[index]).wait()
        here = mine[turn] + jnp.sum(slots[turn, : size_x - 1], axis=0)
        there = jnp.sum(slots[turn, size_x - 1 :], axis=0)
        return [(here[row : row + 1], there[row : row + 1]) for row in range(3)]

    def over(first, second):
        return tuple(a / b for a, b in zip(first, second))

    def curve_of(curved, mixed, ratio, old):
        return tuple(c + b * (2.0 * m + b * o) for c, m, b, o in zip(curved, mixed, ratio, old))

    def inner(first, second):
        return jnp.sum(first * second, axis=0, keepdims=True)

    nothing = jnp.zeros((1, lanes), jnp.float32)

    rhs_move.wait_recv()
    asking = request(0, start_res[...])
    invert_both(mats, pivots, crossing)
    for col in range(2):
        inv_top[col], inv_low[col] = split(mats[col])
    solve(0, *asking, fill_cross)
    apply(0, fill_sides)
    send_far(0, images)
    summing = begin_sum(
        0, [inner(start_res[...], basis[0]), inner(basis[0], images[0]), nothing]
    )
    asking = request(1, images[0])
    solve(1, *asking)
    apply(1)
    send_far(1, images)
    gamma_0, curve_0, _ = end_sum(0, summing)
    alpha_0 = over(gamma_0, curve_0)
    step_0 = alpha_0[0]
    work_image[...] = images[0] - step_0 * images[1]
    asking = request(2, work_image[...])
    work[...] = basis[0] - step_0 * basis[1]
    summing = begin_sum(
        1,
        [
            inner(start_res[...] - step_0 * images[0], work[...]),
            inner(work[...], work_image[...]),
            inner(work[...], images[0]),
        ],
    )
    solve(2, *asking)
    gamma_1, curve_1, mixed_1 = end_sum(1, summing)
    beta_1 = over(gamma_1, gamma_0)
    curve_1 = curve_of(curve_1, mixed_1, beta_1, curve_0)
    alpha_1 = over(gamma_1, curve_1)
    step_1, ratio_1 = alpha_1[0], beta_1[0]

    def prepare():
        old_image[...] = work_image[...] + ratio_1 * images[0]
        last[...] = work[...] - step_1 * (basis[2] + ratio_1 * basis[1])
        work_image[...] = work_image[...] - (step_1 * ratio_1) * images[1]

    apply(2, prepare)
    send_far(2, images)
    last_image = work_image[...] - step_1 * images[2]
    summing = begin_sum(
        2,
        [
            inner(
                start_res[...] - step_0 * images[0] - step_1 * old_image[...], last[...]
            ),
            inner(last[...], last_image),
            inner(last[...], old_image[...]),
        ],
    )
    gamma_2, curve_2, mixed_2 = end_sum(2, summing)
    beta_2 = over(gamma_2, gamma_1)
    curve_2 = curve_of(curve_2, mixed_2, beta_2, curve_1)
    alpha_2 = over(gamma_2, curve_2)

    def weights_of(half_at):
        a_0, a_1, a_2 = alpha_0[half_at], alpha_1[half_at], alpha_2[half_at]
        b_1, b_2 = beta_1[half_at], beta_2[half_at]
        return (
            a_0 + a_1 * (1.0 + b_1) + a_2 * (1.0 + b_2 * (1.0 + b_1)),
            -a_1 * a_0 - a_2 * (a_0 + a_1 * b_1 + b_2 * a_0),
            -a_2 * a_1,
        )

    weights = weights_of(0)
    held = column(my_y)
    solution_ref[:, half(my_y)] = (
        weights[0] * basis[0, held] + weights[1] * basis[1, held] + weights[2] * basis[2, held]
    )
    residual_ref[:, half(my_y)] = start_res[held, :] - (
        weights[0] * images[0, held] + weights[1] * images[1, held] + weights[2] * images[2, held]
    )
    for move in far_moves:
        move.wait_recv()
    weights = weights_of(1)
    solution_ref[:, half(other)] = weights[0] * far[0] + weights[1] * far[1] + weights[2] * far[2]
    residual_ref[:, half(other)] = rhs_ref[:, half(other)] - (
        weights[0] * far[3] + weights[1] * far[4] + weights[2] * far[5]
    )
    for move in pending:
        move.wait_send()


def invert_both(mats, pivots, crossing):
    size, step = mats.shape[1], pivots.shape[1]
    rows = lax.broadcasted_iota(jnp.int32, (size, step), 0)
    lanes = lax.broadcasted_iota(jnp.int32, (size, step), 1)

    def eliminate(index, ahead):
        start = pl.multiple_of(index * step, step)
        here = pl.ds(start, step)
        inside = jnp.logical_and(rows >= start, rows < start + step)
        columns, pivot_rows = [], []
        for which in range(2):
            columns.append(jnp.where(inside, 0.0, mats[which, :, here]))
            mats[which, :, here] = jnp.where(rows - start == lanes, 1.0, 0.0)
            pivot_rows.append(full_dot(pivots[which], mats[which, here, :]))
            mats[which, here, :] = pivot_rows[which]

        def update(which, low):
            part = slice(low, low + step)
            mats[which, part, :] = mats[which, part, :] - full_dot(
                columns[which][part], pivot_rows[which]
            )

        left = [(which, low) for low in range(0, size, step) for which in range(2)]
        if ahead:
            there = pl.ds(pl.multiple_of(start + step, step), step)
            blocks = []
            for which in range(2):
                crossing[which] = columns[which]
                blocks.append(
                    mats[which, there, there]
                    - full_dot(crossing[which, there, :], mats[which, here, there])
                )
            found = pivot_inverses(blocks, lambda: left and update(*left.pop(0)))
        while left:
            update(*left.pop(0))
        for which in range(2):
            mats[which, here, :] = pivot_rows[which]
            if ahead:
                pivots[which] = found[which]

    def looped(index, carry):
        eliminate(index, True)
        return carry

    first = slice(0, step)
    for which, pivot in enumerate(pivot_inverses([mats[at, first, first] for at in range(2)])):
        pivots[which] = pivot
    lax.fori_loop(0, size // step - 1, looped, 0)
    eliminate(size // step - 1, False)


def paired_solve(right_side, coords, noise, intersect):
    points, width = right_side.shape
    size_x = lax.axis_size("gx")
    borrowed = intersect.shape[1]
    lanes, total, ext = width // 2, 2 * points, points + borrowed
    moves = 5 + 1 + ITERS * (2 + 2 + 2 * CUTS + 2 + 1)
    out = jax.ShapeDtypeStruct(right_side.shape, jnp.float32)
    f32 = lambda *shape: pltpu.VMEM(shape, jnp.float32)
    b16 = lambda *shape: pltpu.VMEM(shape, jnp.bfloat16)
    return pl.pallas_call(
        paired_kernel,
        out_shape=(out, out),
        in_specs=[VMEM] * 4,
        out_specs=(VMEM, VMEM),
        scratch_shapes=[
            f32(3, 2, 8, points),
            f32(total, borrowed),
            f32(2, 8, borrowed),
            f32(2, borrowed, borrowed),
            b16(total, 3 * total),
            b16(total, 3 * total),
            f32(2, ext, ext),
            b16(2, ext, ext),
            b16(2, ext, ext),
            b16(6 * borrowed, total),
            b16(total, 6 * borrowed),
            f32(total, lanes),
            f32(ITERS, total, lanes),
            f32(ITERS, total, lanes),
            f32(total, lanes),
            f32(total, lanes),
            f32(total, lanes),
            f32(total, lanes),
            f32(total, 2 * lanes),
            f32(2, ext, 2 * lanes),
            f32(ITERS, 2, 2 * borrowed, lanes),
            f32(2 * borrowed, lanes),
            f32(ITERS, 2, 2 * borrowed, lanes),
            f32(ITERS, 2 * borrowed, lanes),
            f32(ITERS, 2, 2 * borrowed, lanes),
            f32(ITERS, 2, total, lanes),
            f32(2 * ITERS, points, lanes),
            f32(ITERS, 3, lanes),
            f32(ITERS, 2 * size_x - 1, 3, lanes),
            f32(2, borrowed, borrowed),
            f32(2, ext, borrowed),
            pltpu.SemaphoreType.DMA((moves,)),
            pltpu.SemaphoreType.DMA((moves,)),
        ],
        compiler_params=pltpu.CompilerParams(
            collective_id=0, has_side_effects=True, vmem_limit_bytes=58 * 1024 * 1024
        ),
    )(right_side, coords, noise, intersect)


def paired_shards(right_side, coords, noise, intersect):
    points, width = right_side.shape[2:]
    answer, residual = paired_solve(
        right_side.reshape(points, width),
        coords.reshape(2, points),
        noise.reshape(1, points),
        intersect.reshape(1, intersect.shape[2]),
    )
    return answer.reshape(right_side.shape), residual.reshape(right_side.shape)


def solution(mesh):
    placed = (
        P("gx", "gy", None, None),
        P("gx", "gy", None, None),
        P("gx", "gy", None),
        P("gx", "gy", None),
    )
    return jax.shard_map(
        paired_shards if mesh.shape["gy"] == 2 else shards,
        mesh=mesh,
        in_specs=placed,
        out_specs=(P("gx", "gy", None, None), P("gx", "gy", None, None)),
        check_vma=False,
    )
```

```python
import functools
import math

import jax
import jax.numpy as jnp
from jax import lax
from jax.experimental import pallas as pl
from jax.experimental.pallas import tpu as pltpu
from jax.sharding import PartitionSpec as P

ITERS = 3


RANGE_LEN = 0.25
ROOT_THREE = math.sqrt(3.0)
HIGH = lax.Precision.HIGHEST


def shifted(value, axis, by):
    count = lax.axis_size(axis)
    return lax.ppermute(value, axis, [(i, (i + by) % count) for i in range(count)])


def passed_along(block, axis, distance):
    devices = range(lax.axis_size(axis))
    route = [(i - distance, i) for i in devices if i - distance in devices]
    return lax.ppermute(block, axis, route)


def kernel_block(rows_pos, cols_pos):
    delta_x = rows_pos[0][:, None] - cols_pos[0][None, :]
    delta_y = rows_pos[1][:, None] - cols_pos[1][None, :]
    distance = jnp.sqrt(delta_x * delta_x + delta_y * delta_y)
    scaled = ROOT_THREE / RANGE_LEN * distance
    clipped = jnp.minimum(distance, 1.0)
    taper_val = jnp.square(jnp.square(1.0 - clipped)) * (4.0 * clipped + 1.0)
    return (1.0 + scaled) * jnp.exp(-scaled) * taper_val


def window_values(values):
    beside = {}
    for step_by in (1, -1):
        beside[step_by] = shifted(values, "gx", step_by)
    column = jnp.stack([beside[1], values, beside[-1]])
    across = {}
    for step_by in (1, -1):
        across[step_by] = passed_along(column, "gy", step_by)
    return [across[1], column, across[-1]]


CHUNKS = 4
MESH = pl.DeviceIdType.MESH
NOISE_MIN = 0.25
VMEM = pl.BlockSpec(memory_space=pltpu.VMEM)


def split(value):
    top = value.astype(jnp.bfloat16)
    return top, (value - top.astype(jnp.float32)).astype(jnp.bfloat16)


def dot3(left, right):
    left_top, left_low = split(left)
    right_top, right_low = split(right)
    return jnp.dot(
        jnp.concatenate([left_top, left_top, left_low], axis=1),
        jnp.concatenate([right_top, right_low, right_top], axis=0),
        preferred_element_type=jnp.float32,
    )


def dot6(left, right):
    return jnp.dot(left, right, precision=HIGH, preferred_element_type=jnp.float32)


def block_inverse(block):
    size = block.shape[0]
    low, high = NOISE_MIN * 0.97, (size + 1.0) * 1.01
    eye = (
        lax.broadcasted_iota(jnp.int32, block.shape, 0)
        == lax.broadcasted_iota(jnp.int32, block.shape, 1)
    ).astype(jnp.float32)
    first = 2.0 / (low + high)
    gap = 1.0 - first * low
    scale = 2.0 / (2.0 - gap * gap)
    guess = (2.0 * first * scale) * eye - (first * first * scale) * block
    gap = gap * gap / (2.0 - gap * gap)
    while gap > 1e-3:
        scale = 2.0 / (2.0 - gap * gap)
        rest = 2.0 * eye - dot3(block, guess)
        guess = scale * dot3(guess, rest)
        gap = gap * gap / (2.0 - gap * gap)
    for _ in range(2):
        guess = guess + dot3(guess, eye - dot6(block, guess))
    return guess


def invert(matrix_ref, out_ref):
    size = matrix_ref.shape[0]
    step = math.gcd(size, 128)
    out_ref[...] = matrix_ref[...]
    for start in range(0, size, step):
        here = slice(start, start + step)
        pivot = block_inverse(out_ref[here, here])
        column = out_ref[:, here]
        row = dot6(pivot, out_ref[here, :])
        for low in range(0, size, step):
            if low != start:
                part = slice(low, low + step)
                out_ref[part, :] = out_ref[part, :] - dot6(column[part], row)
                out_ref[part, here] = -dot6(column[part], pivot)
        out_ref[here, :] = row
        out_ref[here, here] = pivot


def columns_of(count):
    return () if count == 1 else (1,) if count == 2 else (-1, 1)


def opposite(col_off, count):
    return col_off if count == 2 else -col_off


def offsets_of(count):
    near = [(-1, 0), (1, 0)]
    for col_off in columns_of(count):
        near += [(0, col_off), (-1, col_off), (1, col_off)]
    return near


def cg_kernel(
    rhs_ref, window_ref, matrix_ref, pick_ref, put_ref,
    solution_ref, residual_ref,
    top_ref, low_ref, inverse, inv_top_ref, inv_low_ref, asked, got, tail, back, precond, window, direction, image, mine, slots_y, slots_x,
    send_sem, recv_sem,
):
    size_x, size_y = lax.axis_size("gx"), lax.axis_size("gy")
    my_x, my_y = lax.axis_index("gx"), lax.axis_index("gy")
    near = offsets_of(size_y)
    points = rhs_ref.shape[0]
    borrowed = tail.shape[0]
    half = points // CHUNKS

    def inside(col_off):
        if col_off == 0 or size_y == 2:
            return None
        return my_y > 0 if col_off < 0 else my_y < size_y - 1

    def guarded(condition, action):
        if condition is None:
            action()
        else:
            pl.when(condition)(action)

    def target(row_off, col_off):
        place = {}
        if row_off:
            place["gx"] = lax.rem(my_x + row_off + size_x, size_x)
        if col_off:
            place["gy"] = 1 - my_y if size_y == 2 else my_y + col_off
        return place

    counter = [0]

    class Move:
        def __init__(self, source, dest, row_off, col_off):
            index = counter[0]
            counter[0] += 1
            self.copy = pltpu.make_async_remote_copy(
                src_ref=source,
                dst_ref=dest,
                send_sem=send_sem.at[index],
                recv_sem=recv_sem.at[index],
                device_id=target(row_off, col_off),
                device_id_type=MESH,
            )
            self.out = inside(col_off)
            self.into = inside(-col_off)

        def start(self):
            guarded(self.out, self.copy.start)

        def sent(self):
            guarded(self.out, self.copy.wait_send)

        def landed(self):
            guarded(self.into, self.copy.wait_recv)

    def slot(row_off, col_off):
        return near.index((-row_off, opposite(col_off, size_y)))

    barrier = pltpu.get_barrier_semaphore()
    greeted = 0
    for axis, here, count in (("gx", my_x, size_x), ("gy", my_y, size_y)):
        for hop in range(1, count):
            pl.semaphore_signal(
                barrier, inc=1, device_id={axis: lax.rem(here + hop, count)}, device_id_type=MESH
            )
            greeted += 1
    for row_off, col_off in near:
        if row_off and col_off:

            def greet(row_off=row_off, col_off=col_off):
                pl.semaphore_signal(
                    barrier, inc=1, device_id=target(row_off, col_off), device_id_type=MESH
                )

            guarded(inside(col_off), greet)
            there = inside(col_off)
            greeted = greeted + (1 if there is None else jnp.where(there, 1, 0))

    for col_off in columns_of(size_y):
        there = inside(col_off)
        if there is not None:

            def clear(col_off=col_off):
                for index, (_, col) in enumerate(near):
                    if col == col_off:
                        for iteration in range(ITERS):
                            got[iteration, index] = jnp.zeros(tail.shape, jnp.float32)
                            back[iteration, index] = jnp.zeros(tail.shape, jnp.float32)
                            window[iteration, index] = jnp.zeros(rhs_ref.shape, jnp.float32)

            pl.when(jnp.logical_not(there))(clear)

    def exact_dot(ones, value):
        top, low = split(value)
        return jnp.dot(ones, top, preferred_element_type=jnp.float32) + jnp.dot(
            ones, low, preferred_element_type=jnp.float32
        )

    def dot_parts(left_top, left_low, right):
        right_top, right_low = split(right)
        return (
            jnp.dot(left_top, right_top, preferred_element_type=jnp.float32)
            + jnp.dot(left_top, right_low, preferred_element_type=jnp.float32)
            + jnp.dot(left_low, right_top, preferred_element_type=jnp.float32)
        )

    def window_part(block, value):
        cols = slice(block * points, (block + 1) * points)
        return dot_parts(top_ref[:, cols], low_ref[:, cols], value)

    def total(iteration):
        for stage, (axis, here, count, slots) in enumerate(
            (("gy", my_y, size_y, slots_y), ("gx", my_x, size_x, slots_x))
        ):
            index = counter[0]
            counter[0] += 1
            for hop in range(1, count):
                pltpu.make_async_remote_copy(
                    src_ref=mine.at[iteration, stage],
                    dst_ref=slots.at[iteration, hop - 1],
                    send_sem=send_sem.at[index],
                    recv_sem=recv_sem.at[index],
                    device_id={axis: lax.rem(here + hop, count)},
                    device_id_type=MESH,
                ).start()
            so_far = mine[iteration, stage]
            if count > 1:
                held = slots.at[iteration]
                pltpu.make_async_copy(held, held, recv_sem.at[index]).wait()
                so_far = so_far + jnp.sum(slots[iteration], axis=0)
                pltpu.make_async_copy(held, held, send_sem.at[index]).wait()
            mine[iteration, stage + 1] = so_far
        return mine[iteration, 2]

    residual_ref[...] = rhs_ref[...]
    wait_entry = [True]
    inner_old = denominator = None
    for iteration in range(ITERS):
        requests = exact_dot(pick_ref[...], residual_ref[...])
        for index in range(len(near)):
            asked[index] = requests[index * borrowed : (index + 1) * borrowed]
        if wait_entry[0]:
            pl.semaphore_wait(barrier, greeted)
            wait_entry[0] = False
        moves = [
            Move(asked.at[index], got.at[iteration, slot(*offset)], *offset)
            for index, offset in enumerate(near)
        ]
        for move in moves:
            move.start()
        if iteration == 0:
            invert(matrix_ref, inverse)
            inv_top_ref[...], inv_low_ref[...] = split(inverse[...])
            top_ref[...], low_ref[...] = split(window_ref[...])
        solved = dot_parts(
            inv_top_ref[:, :points], inv_low_ref[:, :points], residual_ref[...]
        )
        for move in moves:
            move.landed()
        gathered = jnp.sum(got[iteration], axis=0)
        solved = solved + dot_parts(inv_top_ref[:, points:], inv_low_ref[:, points:], gathered)
        tail[...] = solved[points:]
        precond[...] = solved[:points]
        returns = [Move(tail, back.at[iteration, slot(*offset)], *offset) for offset in near]
        for move in returns:
            move.start()
        for move in moves:
            move.sent()
        for move in returns:
            move.landed()
        returned = back[iteration].reshape(len(near) * borrowed, tail.shape[1])
        precond[...] = precond[...] + exact_dot(put_ref[...], returned)
        for move in returns:
            move.sent()

        sides, relays = [], []
        for chunk in range(CHUNKS):
            rows = pl.ds(chunk * half, half)
            for col_off in columns_of(size_y):
                index = slot(0, col_off)
                sides.append(
                    Move(precond.at[rows], window.at[iteration, index, rows], 0, col_off)
                )
                sides[-1].start()
        beside = [
            Move(precond, window.at[iteration, slot(row_off, 0)], row_off, 0)
            for row_off in (-1, 1)
        ]
        for move in beside:
            move.start()
        result = window_part(len(near), precond[...])
        place = 0
        for chunk in range(CHUNKS):
            rows = pl.ds(chunk * half, half)
            for col_off in columns_of(size_y):
                sides[place].landed()
                place += 1
                source = near.index((0, opposite(col_off, size_y)))
                for row_off in (-1, 1):
                    index = near.index((-row_off, opposite(col_off, size_y)))
                    move = Move(
                        window.at[iteration, source, rows],
                        window.at[iteration, index, rows],
                        row_off,
                        0,
                    )
                    there = inside(-col_off)
                    move.out = move.into = there
                    relays.append(move)
                    move.start()
        for index, (row_off, col_off) in enumerate(near):
            if row_off == 0:
                result = result + window_part(index, window[iteration, index])
        for move in beside:
            move.landed()
        for index, (row_off, col_off) in enumerate(near):
            if row_off and col_off == 0:
                result = result + window_part(index, window[iteration, index])
        for move in relays:
            move.landed()
        for index, (row_off, col_off) in enumerate(near):
            if row_off and col_off:
                result = result + window_part(index, window[iteration, index])
        fresh = precond[...]
        mine[iteration, 0, 0:1] = jnp.sum(residual_ref[...] * fresh, axis=0, keepdims=True)
        mine[iteration, 0, 1:2] = jnp.sum(fresh * result, axis=0, keepdims=True)
        if iteration:
            mine[iteration, 0, 2:3] = jnp.sum(fresh * image[...], axis=0, keepdims=True)
        else:
            mine[iteration, 0, 2:3] = jnp.zeros((1, fresh.shape[1]), jnp.float32)
        sums = total(iteration)
        for move in sides + beside + relays:
            move.sent()
        inner, curved, mixed = sums[0:1], sums[1:2], sums[2:3]
        if iteration:
            ratio = inner / inner_old
            denominator = curved + ratio * (2.0 * mixed + ratio * denominator)
            direction[...] = fresh + ratio * direction[...]
            image[...] = result + ratio * image[...]
        else:
            denominator = curved
            direction[...] = fresh
            image[...] = result
        inner_old = inner
        step_size = inner / denominator
        moved = step_size * direction[...]
        solution_ref[...] = solution_ref[...] + moved if iteration else moved
        residual_ref[...] = residual_ref[...] - step_size * image[...]


def conjugate_gradients(right_side, window_matrix, matrix, pick):
    near = offsets_of(lax.axis_size("gy"))
    points, width = right_side.shape
    borrowed = matrix.shape[0] - points
    size_x, size_y = lax.axis_size("gx"), lax.axis_size("gy")
    sides = len(columns_of(size_y))
    moves = ITERS * (2 * len(near) + 2 + 3 * CHUNKS * sides + 2)
    out = jax.ShapeDtypeStruct(right_side.shape, jnp.float32)
    block = pltpu.VMEM((points, width), jnp.float32)
    small = (len(near), borrowed, width)
    return pl.pallas_call(
        cg_kernel,
        out_shape=(out, out),
        in_specs=[VMEM] * 5,
        out_specs=(VMEM, VMEM),
        scratch_shapes=[
            pltpu.VMEM(window_matrix.shape, jnp.bfloat16),
            pltpu.VMEM(window_matrix.shape, jnp.bfloat16),
            pltpu.VMEM(matrix.shape, jnp.float32),
            pltpu.VMEM(matrix.shape, jnp.bfloat16),
            pltpu.VMEM(matrix.shape, jnp.bfloat16),
            pltpu.VMEM(small, jnp.float32),
            pltpu.VMEM((ITERS,) + small, jnp.float32),
            pltpu.VMEM((borrowed, width), jnp.float32),
            pltpu.VMEM((ITERS,) + small, jnp.float32),
            block,
            pltpu.VMEM((ITERS, len(near), points, width), jnp.float32),
            block,
            block,
            pltpu.VMEM((ITERS, 3, 3, width), jnp.float32),
            pltpu.VMEM((ITERS, max(size_y - 1, 1), 3, width), jnp.float32),
            pltpu.VMEM((ITERS, max(size_x - 1, 1), 3, width), jnp.float32),
            pltpu.SemaphoreType.DMA((moves,)),
            pltpu.SemaphoreType.DMA((moves,)),
        ],
        compiler_params=pltpu.CompilerParams(
            collective_id=0, has_side_effects=True, vmem_limit_bytes=56 * 1024 * 1024
        ),
    )(right_side, window_matrix, matrix, pick, pick.T)


def shards(right_side, coords, noise, intersect):
    points = right_side.shape[2]
    rhs_count = right_side.shape[3]
    intersect_len = intersect.shape[2]
    ext_len = points + intersect_len
    own_pos = coords.reshape(2, points)
    own_noise = noise.reshape(points)
    listed = jnp.pad(intersect.reshape(intersect_len), (0, points - intersect_len))
    point_info = jnp.concatenate(
        [own_pos, own_noise[None, :], listed.astype(jnp.float32)[None, :]], axis=0
    )
    info_cols = window_values(point_info)
    intersect_ids = intersect.reshape(intersect_len)
    block_id = intersect_ids // points
    row_in = intersect_ids % points
    row_of = block_id // 3
    col_of = block_id % 3
    local_id = row_of * points + row_in
    picked_info = [
        jnp.take(
            jnp.transpose(info_cols[col_off], (1, 0, 2)).reshape(4, 3 * points), local_id, axis=1
        )
        for col_off in range(3)
    ]
    chosen = jnp.where(
        col_of[None, :] == 0,
        picked_info[0],
        jnp.where(col_of[None, :] == 1, picked_info[1], picked_info[2]),
    )
    ov_pos = jnp.stack(
        [chosen[0] + (row_of - 1).astype(jnp.float32), chosen[1] + (col_of - 1).astype(jnp.float32)]
    )
    ext_pos = jnp.concatenate([own_pos, ov_pos], axis=1)
    ext_noise = jnp.concatenate([own_noise, chosen[2]])
    local_matrix = kernel_block(ext_pos, ext_pos) + jnp.diag(ext_noise)
    count = lax.axis_size("gy")
    point_iota = jnp.arange(points, dtype=jnp.int32)[None, :]
    blocks, picks = [], []
    for row_off, col_off in offsets_of(count) + [(0, 0)]:
        step = col_off
        info = info_cols[col_off + 1][row_off + 1]
        if col_off and count == 2:
            first = lax.axis_index("gy") == 0
            step = jnp.where(first, 1, -1)
            info = jnp.where(first, info, info_cols[0][row_off + 1])
        shift = jnp.asarray(step, jnp.float32)
        blocks.append(
            kernel_block(own_pos, jnp.stack([info[0] + float(row_off), info[1] + shift]))
        )
        if row_off or col_off:
            ids = info[3, :intersect_len].astype(jnp.int32)
            own_rows = ids - (3 * (1 - row_off) + (1 - step)) * points
            picks.append((own_rows[:, None] == point_iota).astype(jnp.bfloat16))
    blocks[-1] = blocks[-1] + jnp.diag(own_noise)
    answer, residual = conjugate_gradients(
        right_side.reshape(points, rhs_count),
        jnp.concatenate(blocks, axis=1),
        local_matrix,
        jnp.concatenate(picks, axis=0),
    )
    return (answer.reshape(1, 1, points, rhs_count), residual.reshape(1, 1, points, rhs_count))


def split3(value):
    top = value.astype(jnp.bfloat16)
    rest = value - top.astype(jnp.float32)
    mid = rest.astype(jnp.bfloat16)
    return top, mid, (rest - mid.astype(jnp.float32)).astype(jnp.bfloat16)


def full_dot(left, right):
    lt, lm, ll = split3(left)
    rt, rm, rl = split3(right)
    return jnp.dot(
        jnp.concatenate([lt, lt, lm, lm, lt, ll], axis=1),
        jnp.concatenate([rt, rm, rt, rm, rl, rt], axis=0),
        preferred_element_type=jnp.float32,
    )


def wide(value):
    return jnp.concatenate(split(value), axis=1)


def folded(value):
    lanes = value.shape[1] // 2
    return value[:, :lanes] + value[:, lanes:]


def mm(left, right):
    return jnp.dot(left, right, preferred_element_type=jnp.float32)


def covariance(rows_x, rows_y, cols_x, cols_y):
    rate = ROOT_THREE / RANGE_LEN
    delta_x = rate * rows_x - rate * cols_x
    delta_y = rate * rows_y - rate * cols_y
    square = delta_x * delta_x + delta_y * delta_y
    scaled = square * lax.rsqrt(jnp.maximum(square, 1e-30))
    rest = jnp.maximum(1.0 - (1.0 / rate) * scaled, 0.0)
    rest = rest * rest
    shape = 1.0 + scaled * ((1.0 + 4.0 / rate) + (4.0 / rate) * scaled)
    return shape * jnp.exp(-scaled) * (rest * rest)


def pivot_inverses(blocks, between=lambda: None):
    size = blocks[0].shape[0]
    low, high = NOISE_MIN * 0.97, (size + 1.0) * 1.01
    eye = (
        lax.broadcasted_iota(jnp.int32, blocks[0].shape, 0)
        == lax.broadcasted_iota(jnp.int32, blocks[0].shape, 1)
    ).astype(jnp.float32)
    first = 2.0 / (low + high)
    gap = 1.0 - first * low
    rests = [eye - first * block for block in blocks]
    scale = 2.0 / (2.0 - gap * gap)
    guesses = [(scale * first) * (eye + rest) for rest in rests]
    rests = [scale * dot3(rest, rest) + (1.0 - scale) * eye for rest in rests]
    between()
    gap = gap * gap / (2.0 - gap * gap)
    while True:
        scale = 2.0 / (2.0 - gap * gap)
        gap = gap * gap / (2.0 - gap * gap)
        if gap < 1e-3:
            guesses = [
                scale * (guess + dot3(rest, guess)) for rest, guess in zip(rests, guesses)
            ]
            between()
            break
        both = [
            dot3(rest, jnp.concatenate([rest, guess], axis=1))
            for rest, guess in zip(rests, guesses)
        ]
        guesses = [scale * (guess + pair[:, size:]) for guess, pair in zip(guesses, both)]
        rests = [scale * pair[:, :size] + (1.0 - scale) * eye for pair in both]
        between()
    errors = [eye - full_dot(block, guess) for block, guess in zip(blocks, guesses)]
    between()
    return [guess + dot3(guess, error) for guess, error in zip(guesses, errors)]


SIDES = (-1, 1)
CUTS = 4


def paired_kernel(
    rhs_hbm, coords_ref, noise_ref, ids_ref,
    solution_ref, residual_ref,
    rhs_ref, rhs_sem, info, points_col, ext_row, ext_col, top, low, mats, inv_top, inv_low, pick, put,
    start_res, basis, images, work, work_image, last, old_image, accum, accum_small,
    asked, own_asked, got, tails, back, window, far, mine, slots, pivots, crossing,
    send_sem, recv_sem,
):
    size_x, size_y = lax.axis_size("gx"), lax.axis_size("gy")
    my_x, my_y = lax.axis_index("gx"), lax.axis_index("gy")
    other = 1 - my_y
    points = rhs_ref.shape[0]
    lanes = rhs_ref.shape[1] // 2
    total = 2 * points
    borrowed = ids_ref.shape[1]
    ext = points + borrowed
    row_of_side = {0: 0, -1: 1, 1: 2}

    counter = [0]
    pending = []

    def near(row_off, flip):
        place = {}
        if not isinstance(row_off, int) or row_off:
            place["gx"] = lax.rem(my_x + row_off + size_x, size_x)
        if flip:
            place["gy"] = other
        return place

    def send(source, dest, row_off, flip=False):
        index = counter[0]
        counter[0] += 1
        copy = pltpu.make_async_remote_copy(
            src_ref=source,
            dst_ref=dest,
            send_sem=send_sem.at[index],
            recv_sem=recv_sem.at[index],
            device_id=near(row_off, flip),
            device_id_type=MESH,
        )
        copy.start()
        pending.append(copy)
        return copy

    half = lambda which: pl.ds(pl.multiple_of(which * lanes, lanes), lanes)
    column = lambda which: pl.ds(pl.multiple_of(which * points, points), points)

    loading = pltpu.make_async_copy(rhs_hbm, rhs_ref, rhs_sem)
    loading.start()
    barrier = pltpu.get_barrier_semaphore()
    peers = [(hop, False) for hop in range(1, size_x)] + [(hop, True) for hop in range(size_x)]
    for hop, flip in peers:
        pl.semaphore_signal(barrier, inc=1, device_id=near(hop, flip), device_id_type=MESH)

    info[0, my_y] = jnp.concatenate(
        [
            coords_ref[...],
            noise_ref[...],
            jnp.concatenate(
                [
                    ids_ref[...].astype(jnp.float32),
                    jnp.zeros((1, points - borrowed), jnp.float32),
                ],
                axis=1,
            ),
            jnp.zeros((4, points), jnp.float32),
        ],
        axis=0,
    )
    pl.semaphore_wait(barrier, len(peers))

    facts = []
    for row_off, flip in ((0, True), (-1, False), (1, False), (-1, True), (1, True)):
        dest = info.at[row_of_side[-row_off], my_y]
        facts.append(send(info.at[0, my_y], dest, row_off, flip))
    loading.wait()
    rhs_move = send(rhs_ref.at[:, half(other)], start_res.at[column(my_y), :], 0, True)
    start_res[column(my_y), :] = rhs_ref[:, half(my_y)]

    square_pad = jnp.zeros((borrowed - 8, borrowed), jnp.float32)
    step = 64

    def own_diagonal(start, noise, width):
        here = lax.broadcasted_iota(jnp.int32, (noise.shape[0], width), 0) + start
        across = lax.broadcasted_iota(jnp.int32, (noise.shape[0], width), 1)
        return jnp.where(here == across, noise, 0.0)

    def fill_own(which):
        for low_row in range(0, points, borrowed):
            part = info[0, which][:, low_row : low_row + borrowed]
            rows = pl.ds(pl.multiple_of(which * points + low_row, borrowed), borrowed)
            points_col[rows, :] = jnp.transpose(jnp.concatenate([part, square_pad], axis=0))

        def some(index, carry):
            start = index * step
            rows = pl.ds(pl.multiple_of(which * points + start, step), step)
            block = covariance(
                points_col[rows, 0:1],
                points_col[rows, 1:2],
                info[0, which, 0:1],
                info[0, which, 1:2],
            )
            block = block + own_diagonal(start, points_col[rows, 2:3], points)
            mats[which, pl.ds(pl.multiple_of(start, step), step), 0:points] = block
            cols = column(which)
            top[rows, cols], low[rows, cols] = split(block)
            return carry

        lax.fori_loop(0, points // step, some, 0)

    fill_own(my_y)
    for fact in facts:
        fact.wait_recv()

    def offset_of(row_of, listed_col):
        return float(3 * row_of * points - (listed_col - 1) * points)

    point_down = lax.broadcasted_iota(jnp.int32, (total, borrowed), 0).astype(jnp.float32)
    point_across = lax.broadcasted_iota(jnp.int32, (borrowed, total), 1).astype(jnp.float32)

    def hot(first, second):
        return jnp.where(first == second, 1.0, 0.0).astype(jnp.bfloat16)

    for side in (0, -1, 1):
        place = row_of_side[side]
        for col in range(2):
            facts_here = info[place, col]
            row_ids = facts_here[3:4, :borrowed] - offset_of(1 - side, col)
            slots_here = pl.ds((2 * place + col) * borrowed, borrowed)
            put[:, slots_here] = hot(point_down, row_ids)
            turned = jnp.transpose(
                jnp.concatenate([facts_here[:, :borrowed], square_pad], axis=0)
            )
            pick[slots_here, :] = hot(turned[:, 3:4] - offset_of(1 - side, col), point_across)

    def parts_of(place):
        row = jnp.concatenate([info[place, 0], info[place, 1]], axis=1)
        return jnp.concatenate(
            [part.astype(jnp.float32) for part in split3(row)], axis=0
        ).astype(jnp.bfloat16)

    for col in range(2):
        ids = info[0, col][3:4, :borrowed]
        found = jnp.zeros((24, borrowed), jnp.float32)
        for side in (0, -1, 1):
            place = row_of_side[side]
            found = found + mm(parts_of(place), hot(point_down, ids - offset_of(1 + side, col)))
        found = found[0:8] + found[8:16] + found[16:24]
        row_shift = jnp.where(ids < 3.0 * points, -1.0, jnp.where(ids < 6.0 * points, 0.0, 1.0))
        within = ids - (row_shift + 1.0) * (3.0 * points)
        col_shift = jnp.where(within < points, -1.0, jnp.where(within < 2.0 * points, 0.0, 1.0))
        ext_here = jnp.concatenate(
            [found[0:1] + row_shift, found[1:2] + col_shift, found[2:3], found[3:8]], axis=0
        )
        ext_row[col] = ext_here
        ext_col[col] = jnp.transpose(jnp.concatenate([ext_here, square_pad], axis=0))

    def block_of(rows, col, side, source):
        there = info[row_of_side[side], source]
        return covariance(
            points_col[rows, 0:1],
            points_col[rows, 1:2],
            there[0:1] + float(side),
            there[1:2] + float(source - col),
        )

    def cols_of(side, source):
        at = (2 * row_of_side[side] + source) * points
        return slice(at, at + points)

    def fill(pairs, rows_step):
        for col in range(2):

            def some(index, carry, col=col):
                start = pl.multiple_of(col * points + index * rows_step, rows_step)
                rows = pl.ds(start, rows_step)
                for side, source in pairs(col):
                    cols = cols_of(side, source)
                    top[rows, cols], low[rows, cols] = split(block_of(rows, col, side, source))
                return carry

            lax.fori_loop(0, points // rows_step, some, 0)

    def fill_cross():
        fill(lambda col: [(0, 1 - col)], 64)

    def fill_sides():
        fill(lambda col: [(side, source) for side in SIDES for source in range(2)], 32)

    fill_own(other)
    for col in range(2):

        def fill_ext(index, carry, col=col):
            start = index * step
            rows = pl.ds(pl.multiple_of(start, step), step)
            local = pl.ds(pl.multiple_of(points + start, step), step)
            mine_x = ext_col[col, rows, 0:1]
            mine_y = ext_col[col, rows, 1:2]
            mats[col, local, 0:points] = covariance(
                mine_x, mine_y, info[0, col, 0:1], info[0, col, 1:2]
            )
            block = covariance(mine_x, mine_y, ext_row[col, 0:1], ext_row[col, 1:2])
            mats[col, local, points:ext] = block + own_diagonal(
                start, ext_col[col, rows, 2:3], borrowed
            )
            return carry

        lax.fori_loop(0, borrowed // step, fill_ext, 0)
        mats[col, 0:points, points:ext] = jnp.transpose(mats[col, points:ext, 0:points])

    def joined(first, second, both):
        return mm(
            jnp.concatenate([first, second], axis=1), jnp.concatenate([both, both], axis=0)
        )

    close = 1 - lax.rem(my_x, 2)
    distant = 1 - close

    def request(turn, value):
        both = wide(value)
        moves = []
        for side in (distant, close):
            rows = pl.ds(pl.multiple_of(2 * (1 + side) * borrowed, borrowed), 2 * borrowed)
            asked[turn, side] = folded(mm(pick[rows, :], both))
            moves.append(send(asked.at[turn, side], got.at[turn, 1 - side], 2 * side - 1))
        own_asked[...] = folded(mm(pick[: 2 * borrowed, :], both))
        return both, moves

    piece = total // CUTS

    def solve(turn, both, moves, meanwhile=lambda: None):
        for col in range(2):
            part = both[col * points : (col + 1) * points]
            accum_small[col] = joined(inv_top[col, :, :points], inv_low[col, :, :points], part)
        for move in moves:
            move.wait_recv()
        loaned = []
        for col in range(2):
            rows = slice(col * borrowed, (col + 1) * borrowed)
            loaned.append(wide(own_asked[rows] + got[turn, 0, rows] + got[turn, 1, rows]))
            tails[turn, rows] = folded(
                accum_small[col, points:]
                + joined(inv_top[col, points:, points:], inv_low[col, points:, points:], loaned[col])
            )
        returns = [
            send(tails.at[turn], back.at[turn, 1 - side], 2 * side - 1) for side in (distant, close)
        ]
        owned = mm(put[:, : 2 * borrowed], wide(tails[turn]))
        for col in range(2):
            rows = slice(col * points, (col + 1) * points)
            basis[turn, rows] = folded(
                accum_small[col, :points]
                + joined(inv_top[col, :points, points:], inv_low[col, :points, points:], loaned[col])
                + owned[rows]
            )
        meanwhile()
        for move in returns:
            move.wait_recv()
        came = jnp.concatenate([wide(back[turn, 0]), wide(back[turn, 1])], axis=0)
        moves = []
        for cut in range(CUTS):
            rows = slice(cut * piece, (cut + 1) * piece)
            basis[turn, rows] = basis[turn, rows] + folded(mm(put[rows, 2 * borrowed :], came))
            for side in (distant, close):
                here = pl.ds(cut * piece, piece)
                moves.append(
                    send(basis.at[turn, here], window.at[turn, 1 - side, here], 2 * side - 1)
                )
        return moves

    def apply(turn, moves, meanwhile=lambda: None):
        send_far(turn, basis)
        accum[...] = joined(top[:, :total], low[:, :total], wide(basis[turn]))
        meanwhile()
        for move in moves[1::2]:
            move.wait_recv()
        cols = pl.ds(pl.multiple_of((close + 1) * total, total), total)
        accum[...] = accum[...] + joined(top[:, cols], low[:, cols], wide(window[turn, close]))
        for cut in range(CUTS):
            moves[2 * cut].wait_recv()
            both = wide(window[turn, distant, cut * piece : (cut + 1) * piece])
            cols = pl.ds(pl.multiple_of((distant + 1) * total + cut * piece, piece), piece)
            reached = accum[...] + joined(top[:, cols], low[:, cols], both)
            if cut < CUTS - 1:
                accum[...] = reached
            else:
                images[turn] = folded(reached)

    far_moves = []

    def send_far(turn, source):
        index = turn if source is basis else ITERS + turn
        far_moves.append(send(source.at[turn, column(other)], far.at[index], 0, True))

    def begin_sum(turn, rows):
        mine[turn] = jnp.concatenate(rows, axis=0)
        index = counter[0]
        counter[0] += 1
        for place, (hop, flip) in enumerate(peers):
            pltpu.make_async_remote_copy(
                src_ref=mine.at[turn],
                dst_ref=slots.at[turn, place],
                send_sem=send_sem.at[index],
                recv_sem=recv_sem.at[index],
                device_id=near(hop, flip),
                device_id_type=MESH,
            ).start()
        return index

    def end_sum(turn, index):
        held = slots.at[turn]
        pltpu.make_async_copy(held, held, recv_sem.at[index]).wait()
        pltpu.make_async_copy(held, held, send_sem.at[index]).wait()
        here = mine[turn] + jnp.sum(slots[turn, : size_x - 1], axis=0)
        there = jnp.sum(slots[turn, size_x - 1 :], axis=0)
        return [(here[row : row + 1], there[row : row + 1]) for row in range(3)]

    def over(first, second):
        return tuple(a / b for a, b in zip(first, second))

    def curve_of(curved, mixed, ratio, old):
        return tuple(c + b * (2.0 * m + b * o) for c, m, b, o in zip(curved, mixed, ratio, old))

    def inner(first, second):
        return jnp.sum(first * second, axis=0, keepdims=True)

    nothing = jnp.zeros((1, lanes), jnp.float32)

    rhs_move.wait_recv()
    asking = request(0, start_res[...])
    invert_both(mats, pivots, crossing)
    for col in range(2):
        inv_top[col], inv_low[col] = split(mats[col])
    apply(0, solve(0, *asking, fill_cross), fill_sides)
    send_far(0, images)
    summing = begin_sum(
        0, [inner(start_res[...], basis[0]), inner(basis[0], images[0]), nothing]
    )
    asking = request(1, images[0])
    apply(1, solve(1, *asking))
    send_far(1, images)
    gamma_0, curve_0, _ = end_sum(0, summing)
    alpha_0 = over(gamma_0, curve_0)
    step_0 = alpha_0[0]
    work_image[...] = images[0] - step_0 * images[1]
    asking = request(2, work_image[...])
    work[...] = basis[0] - step_0 * basis[1]
    summing = begin_sum(
        1,
        [
            inner(start_res[...] - step_0 * images[0], work[...]),
            inner(work[...], work_image[...]),
            inner(work[...], images[0]),
        ],
    )
    moves = solve(2, *asking)
    gamma_1, curve_1, mixed_1 = end_sum(1, summing)
    beta_1 = over(gamma_1, gamma_0)
    curve_1 = curve_of(curve_1, mixed_1, beta_1, curve_0)
    alpha_1 = over(gamma_1, curve_1)
    step_1, ratio_1 = alpha_1[0], beta_1[0]

    def prepare():
        old_image[...] = work_image[...] + ratio_1 * images[0]
        last[...] = work[...] - step_1 * (basis[2] + ratio_1 * basis[1])
        work_image[...] = work_image[...] - (step_1 * ratio_1) * images[1]

    apply(2, moves, prepare)
    send_far(2, images)
    last_image = work_image[...] - step_1 * images[2]
    summing = begin_sum(
        2,
        [
            inner(
                start_res[...] - step_0 * images[0] - step_1 * old_image[...], last[...]
            ),
            inner(last[...], last_image),
            inner(last[...], old_image[...]),
        ],
    )
    gamma_2, curve_2, mixed_2 = end_sum(2, summing)
    beta_2 = over(gamma_2, gamma_1)
    curve_2 = curve_of(curve_2, mixed_2, beta_2, curve_1)
    alpha_2 = over(gamma_2, curve_2)

    def weights_of(half_at):
        a_0, a_1, a_2 = alpha_0[half_at], alpha_1[half_at], alpha_2[half_at]
        b_1, b_2 = beta_1[half_at], beta_2[half_at]
        return (
            a_0 + a_1 * (1.0 + b_1) + a_2 * (1.0 + b_2 * (1.0 + b_1)),
            -a_1 * a_0 - a_2 * (a_0 + a_1 * b_1 + b_2 * a_0),
            -a_2 * a_1,
        )

    weights = weights_of(0)
    held = column(my_y)
    solution_ref[:, half(my_y)] = (
        weights[0] * basis[0, held] + weights[1] * basis[1, held] + weights[2] * basis[2, held]
    )
    residual_ref[:, half(my_y)] = start_res[held, :] - (
        weights[0] * images[0, held] + weights[1] * images[1, held] + weights[2] * images[2, held]
    )
    for move in far_moves:
        move.wait_recv()
    weights = weights_of(1)
    solution_ref[:, half(other)] = weights[0] * far[0] + weights[1] * far[1] + weights[2] * far[2]
    residual_ref[:, half(other)] = rhs_ref[:, half(other)] - (
        weights[0] * far[3] + weights[1] * far[4] + weights[2] * far[5]
    )
    for move in pending:
        move.wait_send()


def invert_both(mats, pivots, crossing):
    size, step = mats.shape[1], pivots.shape[1]
    rows = lax.broadcasted_iota(jnp.int32, (size, step), 0)
    lanes = lax.broadcasted_iota(jnp.int32, (size, step), 1)

    def eliminate(index, ahead):
        start = pl.multiple_of(index * step, step)
        here = pl.ds(start, step)
        inside = jnp.logical_and(rows >= start, rows < start + step)
        columns, pivot_rows = [], []
        for which in range(2):
            columns.append(jnp.where(inside, 0.0, mats[which, :, here]))
            mats[which, :, here] = jnp.where(rows - start == lanes, 1.0, 0.0)
            pivot_rows.append(full_dot(pivots[which], mats[which, here, :]))
            mats[which, here, :] = pivot_rows[which]

        def update(which, low):
            part = slice(low, low + step)
            mats[which, part, :] = mats[which, part, :] - full_dot(
                columns[which][part], pivot_rows[which]
            )

        left = [(which, low) for low in range(0, size, step) for which in range(2)]
        if ahead:
            there = pl.ds(pl.multiple_of(start + step, step), step)
            blocks = []
            for which in range(2):
                crossing[which] = columns[which]
                blocks.append(
                    mats[which, there, there]
                    - full_dot(crossing[which, there, :], mats[which, here, there])
                )
            found = pivot_inverses(blocks, lambda: left and update(*left.pop(0)))
        while left:
            update(*left.pop(0))
        for which in range(2):
            mats[which, here, :] = pivot_rows[which]
            if ahead:
                pivots[which] = found[which]

    def looped(index, carry):
        eliminate(index, True)
        return carry

    first = slice(0, step)
    for which, pivot in enumerate(pivot_inverses([mats[at, first, first] for at in range(2)])):
        pivots[which] = pivot
    lax.fori_loop(0, size // step - 1, looped, 0)
    eliminate(size // step - 1, False)


def paired_solve(right_side, coords, noise, intersect):
    points, width = right_side.shape
    size_x = lax.axis_size("gx")
    borrowed = intersect.shape[1]
    lanes, total, ext = width // 2, 2 * points, points + borrowed
    moves = 5 + 1 + ITERS * (2 + 2 + 2 * CUTS + 2 + 1)
    out = jax.ShapeDtypeStruct(right_side.shape, jnp.float32)
    f32 = lambda *shape: pltpu.VMEM(shape, jnp.float32)
    b16 = lambda *shape: pltpu.VMEM(shape, jnp.bfloat16)
    return pl.pallas_call(
        paired_kernel,
        out_shape=(out, out),
        in_specs=[pl.BlockSpec(memory_space=pl.ANY)] + [VMEM] * 3,
        out_specs=(VMEM, VMEM),
        scratch_shapes=[
            f32(points, width),
            pltpu.SemaphoreType.DMA,
            f32(3, 2, 8, points),
            f32(total, borrowed),
            f32(2, 8, borrowed),
            f32(2, borrowed, borrowed),
            b16(total, 3 * total),
            b16(total, 3 * total),
            f32(2, ext, ext),
            b16(2, ext, ext),
            b16(2, ext, ext),
            b16(6 * borrowed, total),
            b16(total, 6 * borrowed),
            f32(total, lanes),
            f32(ITERS, total, lanes),
            f32(ITERS, total, lanes),
            f32(total, lanes),
            f32(total, lanes),
            f32(total, lanes),
            f32(total, lanes),
            f32(total, 2 * lanes),
            f32(2, ext, 2 * lanes),
            f32(ITERS, 2, 2 * borrowed, lanes),
            f32(2 * borrowed, lanes),
            f32(ITERS, 2, 2 * borrowed, lanes),
            f32(ITERS, 2 * borrowed, lanes),
            f32(ITERS, 2, 2 * borrowed, lanes),
            f32(ITERS, 2, total, lanes),
            f32(2 * ITERS, points, lanes),
            f32(ITERS, 3, lanes),
            f32(ITERS, 2 * size_x - 1, 3, lanes),
            f32(2, borrowed, borrowed),
            f32(2, ext, borrowed),
            pltpu.SemaphoreType.DMA((moves,)),
            pltpu.SemaphoreType.DMA((moves,)),
        ],
        compiler_params=pltpu.CompilerParams(
            collective_id=0, has_side_effects=True, vmem_limit_bytes=58 * 1024 * 1024
        ),
    )(right_side, coords, noise, intersect)


def paired_shards(right_side, coords, noise, intersect):
    points, width = right_side.shape[2:]
    answer, residual = paired_solve(
        right_side.reshape(points, width),
        coords.reshape(2, points),
        noise.reshape(1, points),
        intersect.reshape(1, intersect.shape[2]),
    )
    return answer.reshape(right_side.shape), residual.reshape(right_side.shape)


def solution(mesh):
    placed = (
        P("gx", "gy", None, None),
        P("gx", "gy", None, None),
        P("gx", "gy", None),
        P("gx", "gy", None),
    )
    return jax.shard_map(
        paired_shards if mesh.shape["gy"] == 2 and mesh.shape["gx"] % 2 == 0 else shards,
        mesh=mesh,
        in_specs=placed,
        out_specs=(P("gx", "gy", None, None), P("gx", "gy", None, None)),
        check_vma=False,
    )
```

```python
import functools
import math

import jax
import jax.numpy as jnp
from jax import lax
from jax.experimental import pallas as pl
from jax.experimental.pallas import tpu as pltpu
from jax.sharding import PartitionSpec as P

ITERS = 3


RANGE_LEN = 0.25
ROOT_THREE = math.sqrt(3.0)
HIGH = lax.Precision.HIGHEST


def shifted(value, axis, by):
    count = lax.axis_size(axis)
    return lax.ppermute(value, axis, [(i, (i + by) % count) for i in range(count)])


def passed_along(block, axis, distance):
    devices = range(lax.axis_size(axis))
    route = [(i - distance, i) for i in devices if i - distance in devices]
    return lax.ppermute(block, axis, route)


def kernel_block(rows_pos, cols_pos):
    delta_x = rows_pos[0][:, None] - cols_pos[0][None, :]
    delta_y = rows_pos[1][:, None] - cols_pos[1][None, :]
    distance = jnp.sqrt(delta_x * delta_x + delta_y * delta_y)
    scaled = ROOT_THREE / RANGE_LEN * distance
    clipped = jnp.minimum(distance, 1.0)
    taper_val = jnp.square(jnp.square(1.0 - clipped)) * (4.0 * clipped + 1.0)
    return (1.0 + scaled) * jnp.exp(-scaled) * taper_val


def window_values(values):
    beside = {}
    for step_by in (1, -1):
        beside[step_by] = shifted(values, "gx", step_by)
    column = jnp.stack([beside[1], values, beside[-1]])
    across = {}
    for step_by in (1, -1):
        across[step_by] = passed_along(column, "gy", step_by)
    return [across[1], column, across[-1]]


CHUNKS = 4
MESH = pl.DeviceIdType.MESH
NOISE_MIN = 0.25
VMEM = pl.BlockSpec(memory_space=pltpu.VMEM)


def split(value):
    top = value.astype(jnp.bfloat16)
    return top, (value - top.astype(jnp.float32)).astype(jnp.bfloat16)


def dot3(left, right):
    left_top, left_low = split(left)
    right_top, right_low = split(right)
    return jnp.dot(
        jnp.concatenate([left_top, left_top, left_low], axis=1),
        jnp.concatenate([right_top, right_low, right_top], axis=0),
        preferred_element_type=jnp.float32,
    )


def dot6(left, right):
    return jnp.dot(left, right, precision=HIGH, preferred_element_type=jnp.float32)


def block_inverse(block):
    size = block.shape[0]
    low, high = NOISE_MIN * 0.97, (size + 1.0) * 1.01
    eye = (
        lax.broadcasted_iota(jnp.int32, block.shape, 0)
        == lax.broadcasted_iota(jnp.int32, block.shape, 1)
    ).astype(jnp.float32)
    first = 2.0 / (low + high)
    gap = 1.0 - first * low
    scale = 2.0 / (2.0 - gap * gap)
    guess = (2.0 * first * scale) * eye - (first * first * scale) * block
    gap = gap * gap / (2.0 - gap * gap)
    while gap > 1e-3:
        scale = 2.0 / (2.0 - gap * gap)
        rest = 2.0 * eye - dot3(block, guess)
        guess = scale * dot3(guess, rest)
        gap = gap * gap / (2.0 - gap * gap)
    for _ in range(2):
        guess = guess + dot3(guess, eye - dot6(block, guess))
    return guess


def invert(matrix_ref, out_ref):
    size = matrix_ref.shape[0]
    step = math.gcd(size, 128)
    out_ref[...] = matrix_ref[...]
    for start in range(0, size, step):
        here = slice(start, start + step)
        pivot = block_inverse(out_ref[here, here])
        column = out_ref[:, here]
        row = dot6(pivot, out_ref[here, :])
        for low in range(0, size, step):
            if low != start:
                part = slice(low, low + step)
                out_ref[part, :] = out_ref[part, :] - dot6(column[part], row)
                out_ref[part, here] = -dot6(column[part], pivot)
        out_ref[here, :] = row
        out_ref[here, here] = pivot


def columns_of(count):
    return () if count == 1 else (1,) if count == 2 else (-1, 1)


def opposite(col_off, count):
    return col_off if count == 2 else -col_off


def offsets_of(count):
    near = [(-1, 0), (1, 0)]
    for col_off in columns_of(count):
        near += [(0, col_off), (-1, col_off), (1, col_off)]
    return near


def cg_kernel(
    rhs_ref, window_ref, matrix_ref, pick_ref, put_ref,
    solution_ref, residual_ref,
    top_ref, low_ref, inverse, inv_top_ref, inv_low_ref, asked, got, tail, back, precond, window, direction, image, mine, slots_y, slots_x,
    send_sem, recv_sem,
):
    size_x, size_y = lax.axis_size("gx"), lax.axis_size("gy")
    my_x, my_y = lax.axis_index("gx"), lax.axis_index("gy")
    near = offsets_of(size_y)
    points = rhs_ref.shape[0]
    borrowed = tail.shape[0]
    half = points // CHUNKS

    def inside(col_off):
        if col_off == 0 or size_y == 2:
            return None
        return my_y > 0 if col_off < 0 else my_y < size_y - 1

    def guarded(condition, action):
        if condition is None:
            action()
        else:
            pl.when(condition)(action)

    def target(row_off, col_off):
        place = {}
        if row_off:
            place["gx"] = lax.rem(my_x + row_off + size_x, size_x)
        if col_off:
            place["gy"] = 1 - my_y if size_y == 2 else my_y + col_off
        return place

    counter = [0]

    class Move:
        def __init__(self, source, dest, row_off, col_off):
            index = counter[0]
            counter[0] += 1
            self.copy = pltpu.make_async_remote_copy(
                src_ref=source,
                dst_ref=dest,
                send_sem=send_sem.at[index],
                recv_sem=recv_sem.at[index],
                device_id=target(row_off, col_off),
                device_id_type=MESH,
            )
            self.out = inside(col_off)
            self.into = inside(-col_off)

        def start(self):
            guarded(self.out, self.copy.start)

        def sent(self):
            guarded(self.out, self.copy.wait_send)

        def landed(self):
            guarded(self.into, self.copy.wait_recv)

    def slot(row_off, col_off):
        return near.index((-row_off, opposite(col_off, size_y)))

    barrier = pltpu.get_barrier_semaphore()
    greeted = 0
    for axis, here, count in (("gx", my_x, size_x), ("gy", my_y, size_y)):
        for hop in range(1, count):
            pl.semaphore_signal(
                barrier, inc=1, device_id={axis: lax.rem(here + hop, count)}, device_id_type=MESH
            )
            greeted += 1
    for row_off, col_off in near:
        if row_off and col_off:

            def greet(row_off=row_off, col_off=col_off):
                pl.semaphore_signal(
                    barrier, inc=1, device_id=target(row_off, col_off), device_id_type=MESH
                )

            guarded(inside(col_off), greet)
            there = inside(col_off)
            greeted = greeted + (1 if there is None else jnp.where(there, 1, 0))

    for col_off in columns_of(size_y):
        there = inside(col_off)
        if there is not None:

            def clear(col_off=col_off):
                for index, (_, col) in enumerate(near):
                    if col == col_off:
                        for iteration in range(ITERS):
                            got[iteration, index] = jnp.zeros(tail.shape, jnp.float32)
                            back[iteration, index] = jnp.zeros(tail.shape, jnp.float32)
                            window[iteration, index] = jnp.zeros(rhs_ref.shape, jnp.float32)

            pl.when(jnp.logical_not(there))(clear)

    def exact_dot(ones, value):
        top, low = split(value)
        return jnp.dot(ones, top, preferred_element_type=jnp.float32) + jnp.dot(
            ones, low, preferred_element_type=jnp.float32
        )

    def dot_parts(left_top, left_low, right):
        right_top, right_low = split(right)
        return (
            jnp.dot(left_top, right_top, preferred_element_type=jnp.float32)
            + jnp.dot(left_top, right_low, preferred_element_type=jnp.float32)
            + jnp.dot(left_low, right_top, preferred_element_type=jnp.float32)
        )

    def window_part(block, value):
        cols = slice(block * points, (block + 1) * points)
        return dot_parts(top_ref[:, cols], low_ref[:, cols], value)

    def total(iteration):
        for stage, (axis, here, count, slots) in enumerate(
            (("gy", my_y, size_y, slots_y), ("gx", my_x, size_x, slots_x))
        ):
            index = counter[0]
            counter[0] += 1
            for hop in range(1, count):
                pltpu.make_async_remote_copy(
                    src_ref=mine.at[iteration, stage],
                    dst_ref=slots.at[iteration, hop - 1],
                    send_sem=send_sem.at[index],
                    recv_sem=recv_sem.at[index],
                    device_id={axis: lax.rem(here + hop, count)},
                    device_id_type=MESH,
                ).start()
            so_far = mine[iteration, stage]
            if count > 1:
                held = slots.at[iteration]
                pltpu.make_async_copy(held, held, recv_sem.at[index]).wait()
                so_far = so_far + jnp.sum(slots[iteration], axis=0)
                pltpu.make_async_copy(held, held, send_sem.at[index]).wait()
            mine[iteration, stage + 1] = so_far
        return mine[iteration, 2]

    residual_ref[...] = rhs_ref[...]
    wait_entry = [True]
    inner_old = denominator = None
    for iteration in range(ITERS):
        requests = exact_dot(pick_ref[...], residual_ref[...])
        for index in range(len(near)):
            asked[index] = requests[index * borrowed : (index + 1) * borrowed]
        if wait_entry[0]:
            pl.semaphore_wait(barrier, greeted)
            wait_entry[0] = False
        moves = [
            Move(asked.at[index], got.at[iteration, slot(*offset)], *offset)
            for index, offset in enumerate(near)
        ]
        for move in moves:
            move.start()
        if iteration == 0:
            invert(matrix_ref, inverse)
            inv_top_ref[...], inv_low_ref[...] = split(inverse[...])
            top_ref[...], low_ref[...] = split(window_ref[...])
        solved = dot_parts(
            inv_top_ref[:, :points], inv_low_ref[:, :points], residual_ref[...]
        )
        for move in moves:
            move.landed()
        gathered = jnp.sum(got[iteration], axis=0)
        solved = solved + dot_parts(inv_top_ref[:, points:], inv_low_ref[:, points:], gathered)
        tail[...] = solved[points:]
        precond[...] = solved[:points]
        returns = [Move(tail, back.at[iteration, slot(*offset)], *offset) for offset in near]
        for move in returns:
            move.start()
        for move in moves:
            move.sent()
        for move in returns:
            move.landed()
        returned = back[iteration].reshape(len(near) * borrowed, tail.shape[1])
        precond[...] = precond[...] + exact_dot(put_ref[...], returned)
        for move in returns:
            move.sent()

        sides, relays = [], []
        for chunk in range(CHUNKS):
            rows = pl.ds(chunk * half, half)
            for col_off in columns_of(size_y):
                index = slot(0, col_off)
                sides.append(
                    Move(precond.at[rows], window.at[iteration, index, rows], 0, col_off)
                )
                sides[-1].start()
        beside = [
            Move(precond, window.at[iteration, slot(row_off, 0)], row_off, 0)
            for row_off in (-1, 1)
        ]
        for move in beside:
            move.start()
        result = window_part(len(near), precond[...])
        place = 0
        for chunk in range(CHUNKS):
            rows = pl.ds(chunk * half, half)
            for col_off in columns_of(size_y):
                sides[place].landed()
                place += 1
                source = near.index((0, opposite(col_off, size_y)))
                for row_off in (-1, 1):
                    index = near.index((-row_off, opposite(col_off, size_y)))
                    move = Move(
                        window.at[iteration, source, rows],
                        window.at[iteration, index, rows],
                        row_off,
                        0,
                    )
                    there = inside(-col_off)
                    move.out = move.into = there
                    relays.append(move)
                    move.start()
        for index, (row_off, col_off) in enumerate(near):
            if row_off == 0:
                result = result + window_part(index, window[iteration, index])
        for move in beside:
            move.landed()
        for index, (row_off, col_off) in enumerate(near):
            if row_off and col_off == 0:
                result = result + window_part(index, window[iteration, index])
        for move in relays:
            move.landed()
        for index, (row_off, col_off) in enumerate(near):
            if row_off and col_off:
                result = result + window_part(index, window[iteration, index])
        fresh = precond[...]
        mine[iteration, 0, 0:1] = jnp.sum(residual_ref[...] * fresh, axis=0, keepdims=True)
        mine[iteration, 0, 1:2] = jnp.sum(fresh * result, axis=0, keepdims=True)
        if iteration:
            mine[iteration, 0, 2:3] = jnp.sum(fresh * image[...], axis=0, keepdims=True)
        else:
            mine[iteration, 0, 2:3] = jnp.zeros((1, fresh.shape[1]), jnp.float32)
        sums = total(iteration)
        for move in sides + beside + relays:
            move.sent()
        inner, curved, mixed = sums[0:1], sums[1:2], sums[2:3]
        if iteration:
            ratio = inner / inner_old
            denominator = curved + ratio * (2.0 * mixed + ratio * denominator)
            direction[...] = fresh + ratio * direction[...]
            image[...] = result + ratio * image[...]
        else:
            denominator = curved
            direction[...] = fresh
            image[...] = result
        inner_old = inner
        step_size = inner / denominator
        moved = step_size * direction[...]
        solution_ref[...] = solution_ref[...] + moved if iteration else moved
        residual_ref[...] = residual_ref[...] - step_size * image[...]


def conjugate_gradients(right_side, window_matrix, matrix, pick):
    near = offsets_of(lax.axis_size("gy"))
    points, width = right_side.shape
    borrowed = matrix.shape[0] - points
    size_x, size_y = lax.axis_size("gx"), lax.axis_size("gy")
    sides = len(columns_of(size_y))
    moves = ITERS * (2 * len(near) + 2 + 3 * CHUNKS * sides + 2)
    out = jax.ShapeDtypeStruct(right_side.shape, jnp.float32)
    block = pltpu.VMEM((points, width), jnp.float32)
    small = (len(near), borrowed, width)
    return pl.pallas_call(
        cg_kernel,
        out_shape=(out, out),
        in_specs=[VMEM] * 5,
        out_specs=(VMEM, VMEM),
        scratch_shapes=[
            pltpu.VMEM(window_matrix.shape, jnp.bfloat16),
            pltpu.VMEM(window_matrix.shape, jnp.bfloat16),
            pltpu.VMEM(matrix.shape, jnp.float32),
            pltpu.VMEM(matrix.shape, jnp.bfloat16),
            pltpu.VMEM(matrix.shape, jnp.bfloat16),
            pltpu.VMEM(small, jnp.float32),
            pltpu.VMEM((ITERS,) + small, jnp.float32),
            pltpu.VMEM((borrowed, width), jnp.float32),
            pltpu.VMEM((ITERS,) + small, jnp.float32),
            block,
            pltpu.VMEM((ITERS, len(near), points, width), jnp.float32),
            block,
            block,
            pltpu.VMEM((ITERS, 3, 3, width), jnp.float32),
            pltpu.VMEM((ITERS, max(size_y - 1, 1), 3, width), jnp.float32),
            pltpu.VMEM((ITERS, max(size_x - 1, 1), 3, width), jnp.float32),
            pltpu.SemaphoreType.DMA((moves,)),
            pltpu.SemaphoreType.DMA((moves,)),
        ],
        compiler_params=pltpu.CompilerParams(
            collective_id=0, has_side_effects=True, vmem_limit_bytes=56 * 1024 * 1024
        ),
    )(right_side, window_matrix, matrix, pick, pick.T)


def shards(right_side, coords, noise, intersect):
    points = right_side.shape[2]
    rhs_count = right_side.shape[3]
    intersect_len = intersect.shape[2]
    ext_len = points + intersect_len
    own_pos = coords.reshape(2, points)
    own_noise = noise.reshape(points)
    listed = jnp.pad(intersect.reshape(intersect_len), (0, points - intersect_len))
    point_info = jnp.concatenate(
        [own_pos, own_noise[None, :], listed.astype(jnp.float32)[None, :]], axis=0
    )
    info_cols = window_values(point_info)
    intersect_ids = intersect.reshape(intersect_len)
    block_id = intersect_ids // points
    row_in = intersect_ids % points
    row_of = block_id // 3
    col_of = block_id % 3
    local_id = row_of * points + row_in
    picked_info = [
        jnp.take(
            jnp.transpose(info_cols[col_off], (1, 0, 2)).reshape(4, 3 * points), local_id, axis=1
        )
        for col_off in range(3)
    ]
    chosen = jnp.where(
        col_of[None, :] == 0,
        picked_info[0],
        jnp.where(col_of[None, :] == 1, picked_info[1], picked_info[2]),
    )
    ov_pos = jnp.stack(
        [chosen[0] + (row_of - 1).astype(jnp.float32), chosen[1] + (col_of - 1).astype(jnp.float32)]
    )
    ext_pos = jnp.concatenate([own_pos, ov_pos], axis=1)
    ext_noise = jnp.concatenate([own_noise, chosen[2]])
    local_matrix = kernel_block(ext_pos, ext_pos) + jnp.diag(ext_noise)
    count = lax.axis_size("gy")
    point_iota = jnp.arange(points, dtype=jnp.int32)[None, :]
    blocks, picks = [], []
    for row_off, col_off in offsets_of(count) + [(0, 0)]:
        step = col_off
        info = info_cols[col_off + 1][row_off + 1]
        if col_off and count == 2:
            first = lax.axis_index("gy") == 0
            step = jnp.where(first, 1, -1)
            info = jnp.where(first, info, info_cols[0][row_off + 1])
        shift = jnp.asarray(step, jnp.float32)
        blocks.append(
            kernel_block(own_pos, jnp.stack([info[0] + float(row_off), info[1] + shift]))
        )
        if row_off or col_off:
            ids = info[3, :intersect_len].astype(jnp.int32)
            own_rows = ids - (3 * (1 - row_off) + (1 - step)) * points
            picks.append((own_rows[:, None] == point_iota).astype(jnp.bfloat16))
    blocks[-1] = blocks[-1] + jnp.diag(own_noise)
    answer, residual = conjugate_gradients(
        right_side.reshape(points, rhs_count),
        jnp.concatenate(blocks, axis=1),
        local_matrix,
        jnp.concatenate(picks, axis=0),
    )
    return (answer.reshape(1, 1, points, rhs_count), residual.reshape(1, 1, points, rhs_count))


def split3(value):
    top = value.astype(jnp.bfloat16)
    rest = value - top.astype(jnp.float32)
    mid = rest.astype(jnp.bfloat16)
    return top, mid, (rest - mid.astype(jnp.float32)).astype(jnp.bfloat16)


def full_dot(left, right):
    lt, lm, ll = split3(left)
    rt, rm, rl = split3(right)
    return jnp.dot(
        jnp.concatenate([lt, lt, lm, lm, lt, ll], axis=1),
        jnp.concatenate([rt, rm, rt, rm, rl, rt], axis=0),
        preferred_element_type=jnp.float32,
    )


def wide(value):
    return jnp.concatenate(split(value), axis=1)


def folded(value):
    lanes = value.shape[1] // 2
    return value[:, :lanes] + value[:, lanes:]


def mm(left, right):
    return jnp.dot(left, right, preferred_element_type=jnp.float32)


def covariance(rows_x, rows_y, cols_x, cols_y):
    rate = ROOT_THREE / RANGE_LEN
    delta_x = rate * rows_x - rate * cols_x
    delta_y = rate * rows_y - rate * cols_y
    square = delta_x * delta_x + delta_y * delta_y
    scaled = square * lax.rsqrt(jnp.maximum(square, 1e-30))
    rest = jnp.maximum(1.0 - (1.0 / rate) * scaled, 0.0)
    rest = rest * rest
    shape = 1.0 + scaled * ((1.0 + 4.0 / rate) + (4.0 / rate) * scaled)
    return shape * jnp.exp(-scaled) * (rest * rest)


def pivot_inverses(blocks, between=lambda: None):
    size = blocks[0].shape[0]
    low, high = NOISE_MIN * 0.97, (size + 1.0) * 1.01
    eye = (
        lax.broadcasted_iota(jnp.int32, blocks[0].shape, 0)
        == lax.broadcasted_iota(jnp.int32, blocks[0].shape, 1)
    ).astype(jnp.float32)
    first = 2.0 / (low + high)
    gap = 1.0 - first * low
    rests = [eye - first * block for block in blocks]
    scale = 2.0 / (2.0 - gap * gap)
    guesses = [(scale * first) * (eye + rest) for rest in rests]
    rests = [scale * dot3(rest, rest) + (1.0 - scale) * eye for rest in rests]
    between()
    gap = gap * gap / (2.0 - gap * gap)
    while True:
        scale = 2.0 / (2.0 - gap * gap)
        gap = gap * gap / (2.0 - gap * gap)
        if gap < 1e-3:
            guesses = [
                scale * (guess + dot3(rest, guess)) for rest, guess in zip(rests, guesses)
            ]
            between()
            break
        both = [
            dot3(rest, jnp.concatenate([rest, guess], axis=1))
            for rest, guess in zip(rests, guesses)
        ]
        guesses = [scale * (guess + pair[:, size:]) for guess, pair in zip(guesses, both)]
        rests = [scale * pair[:, :size] + (1.0 - scale) * eye for pair in both]
        between()
    errors = [eye - full_dot(block, guess) for block, guess in zip(blocks, guesses)]
    between()
    return [guess + dot3(guess, error) for guess, error in zip(guesses, errors)]


SIDES = (-1, 1)
CUTS = 4


def paired_kernel(
    rhs_hbm, coords_ref, noise_ref, ids_ref,
    solution_ref, residual_ref,
    rhs_ref, rhs_sem, info, points_col, ext_row, ext_col, top, low, mats, inv_top, inv_low, pick, put,
    start_res, basis, images, work, work_image, last, old_image, accum, accum_small,
    asked, own_asked, got, tails, back, window, far, mine, slots, pivots, crossing,
    send_sem, recv_sem,
):
    size_x, size_y = lax.axis_size("gx"), lax.axis_size("gy")
    my_x, my_y = lax.axis_index("gx"), lax.axis_index("gy")
    other = 1 - my_y
    points = rhs_ref.shape[0]
    lanes = rhs_ref.shape[1] // 2
    total = 2 * points
    borrowed = ids_ref.shape[1]
    ext = points + borrowed
    row_of_side = {0: 0, -1: 1, 1: 2}

    counter = [0]
    pending = []

    def near(row_off, flip):
        place = {}
        if not isinstance(row_off, int) or row_off:
            place["gx"] = lax.rem(my_x + row_off + size_x, size_x)
        if flip:
            place["gy"] = other
        return place

    def send(source, dest, row_off, flip=False):
        index = counter[0]
        counter[0] += 1
        copy = pltpu.make_async_remote_copy(
            src_ref=source,
            dst_ref=dest,
            send_sem=send_sem.at[index],
            recv_sem=recv_sem.at[index],
            device_id=near(row_off, flip),
            device_id_type=MESH,
        )
        copy.start()
        pending.append(copy)
        return copy

    half = lambda which: pl.ds(pl.multiple_of(which * lanes, lanes), lanes)
    column = lambda which: pl.ds(pl.multiple_of(which * points, points), points)

    loading = pltpu.make_async_copy(rhs_hbm, rhs_ref, rhs_sem)
    loading.start()
    barrier = pltpu.get_barrier_semaphore()
    peers = [(hop, False) for hop in range(1, size_x)] + [(hop, True) for hop in range(size_x)]
    for hop, flip in peers:
        pl.semaphore_signal(barrier, inc=1, device_id=near(hop, flip), device_id_type=MESH)

    info[0, my_y] = jnp.concatenate(
        [
            coords_ref[...],
            noise_ref[...],
            jnp.concatenate(
                [
                    ids_ref[...].astype(jnp.float32),
                    jnp.zeros((1, points - borrowed), jnp.float32),
                ],
                axis=1,
            ),
            jnp.zeros((4, points), jnp.float32),
        ],
        axis=0,
    )
    pl.semaphore_wait(barrier, len(peers))

    facts = []
    for row_off, flip in ((0, True), (-1, False), (1, False), (-1, True), (1, True)):
        dest = info.at[row_of_side[-row_off], my_y]
        facts.append(send(info.at[0, my_y], dest, row_off, flip))
    loading.wait()
    rhs_move = send(rhs_ref.at[:, half(other)], start_res.at[column(my_y), :], 0, True)
    start_res[column(my_y), :] = rhs_ref[:, half(my_y)]

    square_pad = jnp.zeros((borrowed - 8, borrowed), jnp.float32)
    step = 64

    def own_diagonal(start, noise, width):
        here = lax.broadcasted_iota(jnp.int32, (noise.shape[0], width), 0) + start
        across = lax.broadcasted_iota(jnp.int32, (noise.shape[0], width), 1)
        return jnp.where(here == across, noise, 0.0)

    def fill_own(which):
        for low_row in range(0, points, borrowed):
            part = info[0, which][:, low_row : low_row + borrowed]
            rows = pl.ds(pl.multiple_of(which * points + low_row, borrowed), borrowed)
            points_col[rows, :] = jnp.transpose(jnp.concatenate([part, square_pad], axis=0))

        def some(index, carry):
            start = index * step
            rows = pl.ds(pl.multiple_of(which * points + start, step), step)
            block = covariance(
                points_col[rows, 0:1],
                points_col[rows, 1:2],
                info[0, which, 0:1],
                info[0, which, 1:2],
            )
            block = block + own_diagonal(start, points_col[rows, 2:3], points)
            mats[which, pl.ds(pl.multiple_of(start, step), step), 0:points] = block
            cols = column(which)
            top[rows, cols], low[rows, cols] = split(block)
            return carry

        lax.fori_loop(0, points // step, some, 0)

    fill_own(my_y)
    for fact in facts:
        fact.wait_recv()

    def offset_of(row_of, listed_col):
        return float(3 * row_of * points - (listed_col - 1) * points)

    point_down = lax.broadcasted_iota(jnp.int32, (total, borrowed), 0).astype(jnp.float32)
    point_across = lax.broadcasted_iota(jnp.int32, (borrowed, total), 1).astype(jnp.float32)

    def hot(first, second):
        return jnp.where(first == second, 1.0, 0.0).astype(jnp.bfloat16)

    def mark(side, col):
        place = row_of_side[side]
        facts_here = info[place, col]
        row_ids = facts_here[3:4, :borrowed] - offset_of(1 - side, col)
        slots_here = pl.ds((2 * place + col) * borrowed, borrowed)
        put[:, slots_here] = hot(point_down, row_ids)
        turned = jnp.transpose(jnp.concatenate([facts_here[:, :borrowed], square_pad], axis=0))
        pick[slots_here, :] = hot(turned[:, 3:4] - offset_of(1 - side, col), point_across)

    marks = [(side, col) for side in (0, -1, 1) for col in range(2)]

    def parts_of(place):
        row = jnp.concatenate([info[place, 0], info[place, 1]], axis=1)
        return jnp.concatenate(
            [part.astype(jnp.float32) for part in split3(row)], axis=0
        ).astype(jnp.bfloat16)

    for col in range(2):
        ids = info[0, col][3:4, :borrowed]
        found = jnp.zeros((24, borrowed), jnp.float32)
        for side in (0, -1, 1):
            place = row_of_side[side]
            found = found + mm(parts_of(place), hot(point_down, ids - offset_of(1 + side, col)))
        found = found[0:8] + found[8:16] + found[16:24]
        row_shift = jnp.where(ids < 3.0 * points, -1.0, jnp.where(ids < 6.0 * points, 0.0, 1.0))
        within = ids - (row_shift + 1.0) * (3.0 * points)
        col_shift = jnp.where(within < points, -1.0, jnp.where(within < 2.0 * points, 0.0, 1.0))
        ext_here = jnp.concatenate(
            [found[0:1] + row_shift, found[1:2] + col_shift, found[2:3], found[3:8]], axis=0
        )
        ext_row[col] = ext_here
        ext_col[col] = jnp.transpose(jnp.concatenate([ext_here, square_pad], axis=0))

    def block_of(rows, col, side, source):
        there = info[row_of_side[side], source]
        return covariance(
            points_col[rows, 0:1],
            points_col[rows, 1:2],
            there[0:1] + float(side),
            there[1:2] + float(source - col),
        )

    def cols_of(side, source):
        at = (2 * row_of_side[side] + source) * points
        return slice(at, at + points)

    def fill(pairs, rows_step):
        for col in range(2):

            def some(index, carry, col=col):
                start = pl.multiple_of(col * points + index * rows_step, rows_step)
                rows = pl.ds(start, rows_step)
                for side, source in pairs(col):
                    cols = cols_of(side, source)
                    top[rows, cols], low[rows, cols] = split(block_of(rows, col, side, source))
                return carry

            lax.fori_loop(0, points // rows_step, some, 0)

    def fill_cross():
        fill(lambda col: [(0, 1 - col)], 64)

    def fill_sides():
        fill(lambda col: [(side, source) for side in SIDES for source in range(2)], 64)

    fill_own(other)
    for col in range(2):

        def fill_ext(index, carry, col=col):
            start = index * step
            rows = pl.ds(pl.multiple_of(start, step), step)
            local = pl.ds(pl.multiple_of(points + start, step), step)
            mine_x = ext_col[col, rows, 0:1]
            mine_y = ext_col[col, rows, 1:2]
            mats[col, local, 0:points] = covariance(
                mine_x, mine_y, info[0, col, 0:1], info[0, col, 1:2]
            )
            block = covariance(mine_x, mine_y, ext_row[col, 0:1], ext_row[col, 1:2])
            mats[col, local, points:ext] = block + own_diagonal(
                start, ext_col[col, rows, 2:3], borrowed
            )
            return carry

        lax.fori_loop(0, borrowed // step, fill_ext, 0)
        mats[col, 0:points, points:ext] = jnp.transpose(mats[col, points:ext, 0:points])

    def joined(first, second, both):
        return mm(
            jnp.concatenate([first, second], axis=1), jnp.concatenate([both, both], axis=0)
        )

    close = 1 - lax.rem(my_x, 2)
    distant = 1 - close

    def request(turn, value):
        both = wide(value)
        moves = []
        for side in (distant, close):
            rows = pl.ds(pl.multiple_of(2 * (1 + side) * borrowed, borrowed), 2 * borrowed)
            asked[turn, side] = folded(mm(pick[rows, :], both))
            moves.append(send(asked.at[turn, side], got.at[turn, 1 - side], 2 * side - 1))
        own_asked[...] = folded(mm(pick[: 2 * borrowed, :], both))
        return both, moves

    piece = total // CUTS

    def solve(turn, both, moves, meanwhile=lambda: None):
        for col in range(2):
            part = both[col * points : (col + 1) * points]
            accum_small[col] = joined(inv_top[col, :, :points], inv_low[col, :, :points], part)
        for move in moves:
            move.wait_recv()
        loaned = []
        for col in range(2):
            rows = slice(col * borrowed, (col + 1) * borrowed)
            loaned.append(wide(own_asked[rows] + got[turn, 0, rows] + got[turn, 1, rows]))
            tails[turn, rows] = folded(
                accum_small[col, points:]
                + joined(inv_top[col, points:, points:], inv_low[col, points:, points:], loaned[col])
            )
        returns = [
            send(tails.at[turn], back.at[turn, 1 - side], 2 * side - 1) for side in (distant, close)
        ]
        owned = mm(put[:, : 2 * borrowed], wide(tails[turn]))
        for col in range(2):
            rows = slice(col * points, (col + 1) * points)
            basis[turn, rows] = folded(
                accum_small[col, :points]
                + joined(inv_top[col, :points, points:], inv_low[col, :points, points:], loaned[col])
                + owned[rows]
            )
        meanwhile()
        for move in returns:
            move.wait_recv()
        came = jnp.concatenate([wide(back[turn, 0]), wide(back[turn, 1])], axis=0)
        moves = []
        for cut in range(CUTS):
            rows = slice(cut * piece, (cut + 1) * piece)
            basis[turn, rows] = basis[turn, rows] + folded(mm(put[rows, 2 * borrowed :], came))
            for side in (distant, close):
                here = pl.ds(cut * piece, piece)
                moves.append(
                    send(basis.at[turn, here], window.at[turn, 1 - side, here], 2 * side - 1)
                )
        return moves

    def apply(turn, moves, meanwhile=lambda: None):
        send_far(turn, basis)
        accum[...] = joined(top[:, :total], low[:, :total], wide(basis[turn]))
        meanwhile()
        for move in moves[1::2]:
            move.wait_recv()
        cols = pl.ds(pl.multiple_of((close + 1) * total, total), total)
        accum[...] = accum[...] + joined(top[:, cols], low[:, cols], wide(window[turn, close]))
        for cut in range(CUTS):
            moves[2 * cut].wait_recv()
            both = wide(window[turn, distant, cut * piece : (cut + 1) * piece])
            cols = pl.ds(pl.multiple_of((distant + 1) * total + cut * piece, piece), piece)
            reached = accum[...] + joined(top[:, cols], low[:, cols], both)
            if cut < CUTS - 1:
                accum[...] = reached
            else:
                images[turn] = folded(reached)

    far_moves = []

    def send_far(turn, source):
        index = turn if source is basis else ITERS + turn
        far_moves.append(send(source.at[turn, column(other)], far.at[index], 0, True))

    def begin_sum(turn, rows):
        mine[turn] = jnp.concatenate(rows, axis=0)
        index = counter[0]
        counter[0] += 1
        for place, (hop, flip) in enumerate(peers):
            pltpu.make_async_remote_copy(
                src_ref=mine.at[turn],
                dst_ref=slots.at[turn, place],
                send_sem=send_sem.at[index],
                recv_sem=recv_sem.at[index],
                device_id=near(hop, flip),
                device_id_type=MESH,
            ).start()
        return index

    def end_sum(turn, index):
        held = slots.at[turn]
        pltpu.make_async_copy(held, held, recv_sem.at[index]).wait()
        pltpu.make_async_copy(held, held, send_sem.at[index]).wait()
        here = mine[turn] + jnp.sum(slots[turn, : size_x - 1], axis=0)
        there = jnp.sum(slots[turn, size_x - 1 :], axis=0)
        return [(here[row : row + 1], there[row : row + 1]) for row in range(3)]

    def over(first, second):
        return tuple(a / b for a, b in zip(first, second))

    def curve_of(curved, mixed, ratio, old):
        return tuple(c + b * (2.0 * m + b * o) for c, m, b, o in zip(curved, mixed, ratio, old))

    def inner(first, second):
        return jnp.sum(first * second, axis=0, keepdims=True)

    nothing = jnp.zeros((1, lanes), jnp.float32)

    def ask_first():
        rhs_move.wait_recv()
        return request(0, start_res[...])

    asking = invert_both(
        mats, pivots, crossing, lambda: marks and mark(*marks.pop(0)), ask_first
    )
    for col in range(2):
        inv_top[col], inv_low[col] = split(mats[col])
    apply(0, solve(0, *asking, fill_cross), fill_sides)
    send_far(0, images)
    summing = begin_sum(
        0, [inner(start_res[...], basis[0]), inner(basis[0], images[0]), nothing]
    )
    asking = request(1, images[0])
    apply(1, solve(1, *asking))
    send_far(1, images)
    gamma_0, curve_0, _ = end_sum(0, summing)
    alpha_0 = over(gamma_0, curve_0)
    step_0 = alpha_0[0]
    work_image[...] = images[0] - step_0 * images[1]
    asking = request(2, work_image[...])
    work[...] = basis[0] - step_0 * basis[1]
    summing = begin_sum(
        1,
        [
            inner(start_res[...] - step_0 * images[0], work[...]),
            inner(work[...], work_image[...]),
            inner(work[...], images[0]),
        ],
    )
    moves = solve(2, *asking)
    gamma_1, curve_1, mixed_1 = end_sum(1, summing)
    beta_1 = over(gamma_1, gamma_0)
    curve_1 = curve_of(curve_1, mixed_1, beta_1, curve_0)
    alpha_1 = over(gamma_1, curve_1)
    step_1, ratio_1 = alpha_1[0], beta_1[0]

    def prepare():
        old_image[...] = work_image[...] + ratio_1 * images[0]
        last[...] = work[...] - step_1 * (basis[2] + ratio_1 * basis[1])
        work_image[...] = work_image[...] - (step_1 * ratio_1) * images[1]

    apply(2, moves, prepare)
    send_far(2, images)
    last_image = work_image[...] - step_1 * images[2]
    summing = begin_sum(
        2,
        [
            inner(
                start_res[...] - step_0 * images[0] - step_1 * old_image[...], last[...]
            ),
            inner(last[...], last_image),
            inner(last[...], old_image[...]),
        ],
    )
    gamma_2, curve_2, mixed_2 = end_sum(2, summing)
    beta_2 = over(gamma_2, gamma_1)
    curve_2 = curve_of(curve_2, mixed_2, beta_2, curve_1)
    alpha_2 = over(gamma_2, curve_2)

    def weights_of(half_at):
        a_0, a_1, a_2 = alpha_0[half_at], alpha_1[half_at], alpha_2[half_at]
        b_1, b_2 = beta_1[half_at], beta_2[half_at]
        return (
            a_0 + a_1 * (1.0 + b_1) + a_2 * (1.0 + b_2 * (1.0 + b_1)),
            -a_1 * a_0 - a_2 * (a_0 + a_1 * b_1 + b_2 * a_0),
            -a_2 * a_1,
        )

    weights = weights_of(0)
    held = column(my_y)
    solution_ref[:, half(my_y)] = (
        weights[0] * basis[0, held] + weights[1] * basis[1, held] + weights[2] * basis[2, held]
    )
    residual_ref[:, half(my_y)] = start_res[held, :] - (
        weights[0] * images[0, held] + weights[1] * images[1, held] + weights[2] * images[2, held]
    )
    for move in far_moves:
        move.wait_recv()
    weights = weights_of(1)
    solution_ref[:, half(other)] = weights[0] * far[0] + weights[1] * far[1] + weights[2] * far[2]
    residual_ref[:, half(other)] = rhs_ref[:, half(other)] - (
        weights[0] * far[3] + weights[1] * far[4] + weights[2] * far[5]
    )
    for move in pending:
        move.wait_send()


def invert_both(mats, pivots, crossing, beside, meanwhile):
    size, step = mats.shape[1], pivots.shape[1]
    rows = lax.broadcasted_iota(jnp.int32, (size, step), 0)
    lanes = lax.broadcasted_iota(jnp.int32, (size, step), 1)

    def eliminate(index, ahead):
        start = pl.multiple_of(index * step, step)
        here = pl.ds(start, step)
        inside = jnp.logical_and(rows >= start, rows < start + step)
        columns, pivot_rows = [], []
        for which in range(2):
            columns.append(jnp.where(inside, 0.0, mats[which, :, here]))
            mats[which, :, here] = jnp.where(rows - start == lanes, 1.0, 0.0)
            pivot_rows.append(full_dot(pivots[which], mats[which, here, :]))
            mats[which, here, :] = pivot_rows[which]

        def update(which, low):
            part = slice(low, low + step)
            mats[which, part, :] = mats[which, part, :] - full_dot(
                columns[which][part], pivot_rows[which]
            )

        left = [(which, low) for low in range(0, size, step) for which in range(2)]
        if ahead:
            there = pl.ds(pl.multiple_of(start + step, step), step)
            blocks = []
            for which in range(2):
                crossing[which] = columns[which]
                blocks.append(
                    mats[which, there, there]
                    - full_dot(crossing[which, there, :], mats[which, here, there])
                )
            found = pivot_inverses(blocks, lambda: left and update(*left.pop(0)))
        while left:
            update(*left.pop(0))
        for which in range(2):
            mats[which, here, :] = pivot_rows[which]
            if ahead:
                pivots[which] = found[which]

    def looped(index, carry):
        eliminate(index, True)
        return carry

    first = slice(0, step)
    found = pivot_inverses([mats[which, first, first] for which in range(2)], beside)
    for which in range(2):
        pivots[which] = found[which]
    last = size // step - 1
    lax.fori_loop(0, last // 2, looped, 0)
    result = meanwhile()
    lax.fori_loop(last // 2, last, looped, 0)
    eliminate(last, False)
    return result


def paired_solve(right_side, coords, noise, intersect):
    points, width = right_side.shape
    size_x = lax.axis_size("gx")
    borrowed = intersect.shape[1]
    lanes, total, ext = width // 2, 2 * points, points + borrowed
    moves = 5 + 1 + ITERS * (2 + 2 + 2 * CUTS + 2 + 1)
    out = jax.ShapeDtypeStruct(right_side.shape, jnp.float32)
    f32 = lambda *shape: pltpu.VMEM(shape, jnp.float32)
    b16 = lambda *shape: pltpu.VMEM(shape, jnp.bfloat16)
    return pl.pallas_call(
        paired_kernel,
        out_shape=(out, out),
        in_specs=[pl.BlockSpec(memory_space=pltpu.HBM)] + [VMEM] * 3,
        out_specs=(VMEM, VMEM),
        scratch_shapes=[
            f32(points, width),
            pltpu.SemaphoreType.DMA,
            f32(3, 2, 8, points),
            f32(total, borrowed),
            f32(2, 8, borrowed),
            f32(2, borrowed, borrowed),
            b16(total, 3 * total),
            b16(total, 3 * total),
            f32(2, ext, ext),
            b16(2, ext, ext),
            b16(2, ext, ext),
            b16(6 * borrowed, total),
            b16(total, 6 * borrowed),
            f32(total, lanes),
            f32(ITERS, total, lanes),
            f32(ITERS, total, lanes),
            f32(total, lanes),
            f32(total, lanes),
            f32(total, lanes),
            f32(total, lanes),
            f32(total, 2 * lanes),
            f32(2, ext, 2 * lanes),
            f32(ITERS, 2, 2 * borrowed, lanes),
            f32(2 * borrowed, lanes),
            f32(ITERS, 2, 2 * borrowed, lanes),
            f32(ITERS, 2 * borrowed, lanes),
            f32(ITERS, 2, 2 * borrowed, lanes),
            f32(ITERS, 2, total, lanes),
            f32(2 * ITERS, points, lanes),
            f32(ITERS, 3, lanes),
            f32(ITERS, 2 * size_x - 1, 3, lanes),
            f32(2, borrowed, borrowed),
            f32(2, ext, borrowed),
            pltpu.SemaphoreType.DMA((moves,)),
            pltpu.SemaphoreType.DMA((moves,)),
        ],
        compiler_params=pltpu.CompilerParams(
            collective_id=0, has_side_effects=True, vmem_limit_bytes=52 * 1024 * 1024
        ),
    )(right_side, coords, noise, intersect)


def paired_shards(right_side, coords, noise, intersect):
    points, width = right_side.shape[2:]
    answer, residual = paired_solve(
        right_side.reshape(points, width),
        coords.reshape(2, points),
        noise.reshape(1, points),
        intersect.reshape(1, intersect.shape[2]),
    )
    return answer.reshape(right_side.shape), residual.reshape(right_side.shape)


def solution(mesh):
    placed = (
        P("gx", "gy", None, None),
        P("gx", "gy", None, None),
        P("gx", "gy", None),
        P("gx", "gy", None),
    )
    return jax.shard_map(
        paired_shards if mesh.shape["gy"] == 2 and mesh.shape["gx"] % 2 == 0 else shards,
        mesh=mesh,
        in_specs=placed,
        out_specs=(P("gx", "gy", None, None), P("gx", "gy", None, None)),
        check_vma=False,
    )
```
